32 devices in a mesh: dp: 8 (over z, core), tensor: 4 (over y, x).
Axes of the slice: x: 2, y: 2, z: 4, core: 2. Of those that a mesh axis runs over, the one named last changes fastest.
Arguments:
- hidden_in: bfloat16 [8192, 5120], P(('dp', 'tensor')), may hold values from -64 to 64
- q_weight: bfloat16 [5120, 1024], P('dp', 'tensor'), may hold values from -0.69877124 to 0.69877124
- k_weight: bfloat16 [5120, 1024], P('dp'), may hold values from -0.69877124 to 0.69877124
- v_weight: bfloat16 [5120, 1024], P('dp'), may hold values from -0.078125 to 0.078125
- q_gain: float32 [1024], P('tensor'), may hold values from 0.1 to 1.9
- k_gain: float32 [1024], replicated, may hold values from 0.1 to 1.9
- o_weight: bfloat16 [1024, 5120], P('tensor', 'dp'), may hold values from -0.1875 to 0.1875
- post_gain: float32 [5120], replicated, may hold values from 0.1 to 1.9
Outputs:
- layer_out: bfloat16 [8192, 5120], P(('dp', 'tensor'))
The draws below stay inside these ranges and needn't reach their ends.
All inputs are finite; a program needn't handle non-finite values.
Results may differ from the reference program's by a relative error of at most 0.012.
Values may be sent and summed in bfloat16 or wider, within the bound.
A program may use at most 128 MiB of HBM per device.

```python
import jax
import jax.numpy as jnp
from jax import lax

D = 5120
HD = 128
KV_HEADS = 8
HEADS_DEV = 2
SEQ = 1024
HEADS = 8
TOKENS = 8192
N_DP = 8


def clipped(key, shape):
    return jnp.clip(jax.random.normal(key, shape, jnp.float32), -6.0, 6.0)


def head_scales(key, count):
    ramp = jnp.exp(0.5 * jnp.log(3.0) * jnp.arange(count, dtype=jnp.float32) / (count - 1))
    return ramp * jax.random.uniform(key, (count,), jnp.float32, 0.7, 1.3)


def draw_hidden_in(key, part):
    base = clipped(jax.random.fold_in(key, 1), (TOKENS, D))
    return base.astype(jnp.bfloat16)


def draw_k_weight(key, part):
    base = clipped(jax.random.fold_in(key, 3), (D, KV_HEADS * HD)) * D ** (-0.5)
    return base.astype(jnp.bfloat16)


def draw_q_weight(key, part):
    base = clipped(jax.random.fold_in(key, 4), (D, HEADS, HD)) * D ** (-0.5)
    base = base * head_scales(jax.random.fold_in(key, 6), HEADS)[None, :, None]
    base = base.reshape(D, HEADS * HD)
    return base.astype(jnp.bfloat16)


def level_of(stream_key, dims, cuts, low, high):
    def one(position, parts):
        heights = jax.random.uniform(jax.random.fold_in(jax.random.fold_in(stream_key, 6), position), (parts,), jnp.float32, low / len(cuts), high / len(cuts))
        return jnp.repeat(jnp.exp(heights), dims[position] // parts).reshape((-1,) + (1,) * (len(dims) - position - 1))

    loudness = one(*cuts[0])
    for cut in cuts[1:]:
        loudness = loudness * one(*cut)
    return loudness


def normal_values(rng, dims, deviation, limit, pieces=(), kind=jnp.bfloat16):
    entries = deviation * jax.random.normal(rng, dims, jnp.float32)
    if pieces:
        entries = entries * level_of(rng, dims, pieces, -0.22, 0.18)
    return jnp.clip(entries, -limit, limit).astype(kind)


def setup_inputs(seed: int = 0) -> dict:
    keys = jax.random.split(jax.random.key(seed), 9)
    hidden_in = draw_hidden_in(jax.random.fold_in(keys[8], 71), 0)
    q_weight = draw_q_weight(jax.random.fold_in(keys[8], 71), 0)
    k_weight = draw_k_weight(jax.random.fold_in(keys[8], 71), 0)
    v_weight = normal_values(keys[3], (D, KV_HEADS * HD), D ** -0.5, 0.078125, ((0, 8),))
    q_gain = jnp.clip(1.0 + 0.18 * jax.random.normal(keys[4], (HEADS * HD,), jnp.float32), 0.1, 1.9)
    k_gain = jnp.clip(1.0 + 0.18 * jax.random.normal(keys[5], (KV_HEADS * HD,), jnp.float32), 0.1, 1.9)
    o_weight = normal_values(keys[6], (HEADS * HD, D), (HEADS * HD) ** -0.5, 0.1875, ((0, 4), (1, 8)))
    post_gain = jnp.clip(1.0 + 0.18 * jax.random.normal(keys[7], (D,), jnp.float32), 0.1, 1.9)
    return dict(hidden_in=hidden_in, q_weight=q_weight, k_weight=k_weight, v_weight=v_weight, q_gain=q_gain, k_gain=k_gain, o_weight=o_weight, post_gain=post_gain)


epsilon = 1e-06

def rms_scale(block, gain, width):
    mean_square = lax.optimization_barrier(jnp.sum(block * block, axis=1, keepdims=True)) / width
    return block * lax.rsqrt(mean_square + epsilon) * gain

def one_sequence(tokens, q_weight, k_weight, v_weight, q_gain, k_gain, o_weight, post_gain):
    queries = jnp.dot(tokens, q_weight, preferred_element_type=jnp.float32)
    key_rows = jnp.dot(tokens, k_weight, preferred_element_type=jnp.float32)
    value_rows = jnp.dot(tokens, v_weight, preferred_element_type=jnp.float32).astype(jnp.bfloat16)
    q_normed = rms_scale(queries, q_gain, HEADS * HD).astype(jnp.bfloat16)
    k_normed = rms_scale(key_rows, k_gain, KV_HEADS * HD).astype(jnp.bfloat16)
    group_size = HEADS // KV_HEADS
    q_heads = q_normed.astype(jnp.float32).reshape(SEQ, HEADS, HD)
    k_heads = jnp.repeat(k_normed.astype(jnp.float32).reshape(SEQ, KV_HEADS, HD), group_size, axis=1)
    v_heads = jnp.repeat(value_rows.astype(jnp.float32).reshape(SEQ, KV_HEADS, HD), group_size, axis=1)
    scores = jnp.einsum('qhd,khd->hqk', q_heads, k_heads) * HD ** (-0.5)
    rows_idx = lax.broadcasted_iota(jnp.int32, (SEQ, SEQ), 0)
    cols_idx = lax.broadcasted_iota(jnp.int32, (SEQ, SEQ), 1)
    scores = jnp.where((cols_idx <= rows_idx)[None], scores, -1e+30)
    row_max = lax.optimization_barrier(jnp.max(scores, axis=-1, keepdims=True))
    expo = jnp.exp(scores - row_max)
    soft_weights = (expo / lax.optimization_barrier(jnp.sum(expo, axis=-1, keepdims=True))).astype(jnp.bfloat16)
    attended = jnp.einsum('hqk,khd->qhd', soft_weights.astype(jnp.float32), v_heads).astype(jnp.bfloat16)
    blocks = HEADS // HEADS_DEV
    attended_blocks = attended.reshape(SEQ, blocks, HEADS_DEV * HD).astype(jnp.float32)
    weight_blocks = o_weight.reshape(blocks, HEADS_DEV * HD, D).astype(jnp.float32)
    partials = jnp.einsum('snk,nkd->nsd', attended_blocks, weight_blocks)
    rounded = lax.optimization_barrier(partials.astype(jnp.bfloat16)).astype(jnp.float32)
    projected = lax.optimization_barrier(jnp.sum(rounded, axis=0))
    mean_square = lax.optimization_barrier(jnp.mean(projected * projected, axis=1, keepdims=True))
    result = tokens.astype(jnp.float32) + projected * lax.rsqrt(mean_square + epsilon) * post_gain
    return result.astype(jnp.bfloat16)

def reference(hidden_in, q_weight, k_weight, v_weight, q_gain, k_gain, o_weight, post_gain):
    sequences = hidden_in.reshape(N_DP, SEQ, D)

    def apply_layer(tokens):
        return one_sequence(tokens, q_weight, k_weight, v_weight, q_gain, k_gain, o_weight, post_gain)
    outputs = lax.map(apply_layer, sequences)
    return outputs.reshape(TOKENS, D)
```

```python
import functools

import jax
import jax.numpy as jnp
from jax import lax
from jax.experimental import pallas as pl
from jax.experimental.pallas import tpu as pltpu
from jax.sharding import PartitionSpec as P

HD = 128
KV_HEADS = 8
CORES = 2
MESH = pl.DeviceIdType.MESH

epsilon = 1e-06


def plane_of(tensor_size):
    ny = max(n for n in range(1, tensor_size + 1) if tensor_size % n == 0 and n * n <= tensor_size)
    return ny, tensor_size // ny


class Copies:
    def __init__(self, send_sem, recv_sem):
        self.send_sem, self.recv_sem, self.count, self.sent = send_sem, recv_sem, 0, []

    def slot(self):
        self.count += 1
        return self.count - 1

    def make(self, slot, src, dst, device):
        return pltpu.make_async_remote_copy(
            src_ref=src,
            dst_ref=dst,
            send_sem=self.send_sem.at[slot],
            recv_sem=self.recv_sem.at[slot],
            device_id=device,
            device_id_type=MESH,
        )

    def send(self, slot, src, dst, device, when=None):
        copy = self.make(slot, src, dst, device)
        self.sent.append((copy, when))
        run(when, copy.start)

    def receive(self, slot, dst, device, when=None):
        run(when, self.make(slot, dst, dst, device).wait_recv)

    def finish(self):
        for copy, when in self.sent:
            run(when, copy.wait_send)


def run(when, action):
    if when is None:
        action()
    else:
        pl.when(when)(action)


def gather_kernel(
    plan, hid, qw, kw, vw, ow, tok, wts, full, hid_v, w_v, o_v, local_sem, send_sem, recv_sem
):
    ny, nx, nz, q_width, kv_width, kv_step, group = plan
    t, d = lax.axis_index("tensor"), lax.axis_index("dp")
    tx, ty = lax.rem(t, nx), lax.div(t, nx)
    c, z = lax.rem(d, CORES), lax.div(d, CORES)
    rows, depth = hid.shape[0], qw.shape[0]
    o_rows, o_cols = ow.shape
    copies = Copies(send_sem, recv_sem)

    def at_x(j):
        return {"tensor": ty * nx + lax.rem(tx + j, nx), "dp": d}

    def at_y(j):
        return {"tensor": lax.rem(ty + j, ny) * nx + tx, "dp": d}

    up = {"tensor": t, "dp": jnp.minimum(d + CORES, nz * CORES - 1)}
    down = {"tensor": t, "dp": jnp.maximum(d - CORES, 0)}
    partner = {"tensor": t, "dp": z * CORES + 1 - c}
    has_up, has_down = z + 1 < nz, z > 0

    kv_first = pl.multiple_of(lax.div(t * kv_step, group) * HD, HD)
    loads = [
        pltpu.make_async_copy(qw, w_v.at[:, pl.ds(0, q_width)], local_sem.at[0]),
        pltpu.make_async_copy(
            kw.at[:, pl.ds(kv_first, kv_width)], w_v.at[:, pl.ds(q_width, kv_width)], local_sem.at[1]
        ),
        pltpu.make_async_copy(
            vw.at[:, pl.ds(kv_first, kv_width)],
            w_v.at[:, pl.ds(q_width + kv_width, kv_width)],
            local_sem.at[2],
        ),
        pltpu.make_async_copy(hid, hid_v, local_sem.at[3]),
        pltpu.make_async_copy(ow, o_v, local_sem.at[4]),
    ]
    for load in loads:
        load.start()

    barrier = pltpu.get_barrier_semaphore()

    def greet(device):
        pl.semaphore_signal(barrier, inc=1, device_id=device, device_id_type=MESH)

    for j in range(1, nx):
        greet(at_x(j))
    for j in range(1, ny):
        greet(at_y(j))
    greet(partner)
    run(has_up, lambda: greet(up))
    run(has_down, lambda: greet(down))
    pl.semaphore_wait(
        barrier, nx + ny - 1 + has_up.astype(jnp.int32) + has_down.astype(jnp.int32)
    )

    def w_at(dp):
        return wts.at[pl.ds(pl.multiple_of(dp * depth, 8), depth), :]

    def o_at(tensor, dp, part=None):
        size = o_rows if part is None else o_rows // 2
        start = tensor * o_rows + (0 if part is None else part * size)
        return full.at[dp, pl.ds(pl.multiple_of(start, 8), size), :]

    def tok_at(tensor, part):
        size = rows // 2
        return tok.at[pl.ds(pl.multiple_of(tensor * rows + part * size, 8), size), :]

    for load in loads:
        load.wait()
    line = {}
    for name in ("w", "o"):
        for way in ("up", "down"):
            for s in range(1, nz):
                line[name, way, s] = copies.slot()
    links = (("up", up, has_up, 1), ("down", down, has_down, -1))
    for way, device, has, sign in links:
        copies.send(line["w", way, 1], w_v, w_at(d), device, has)

    class Plane:
        def __init__(self, at):
            self.at = at
            self.first = {(p, j): copies.slot() for p in (0, 1) for j in range(1, (nx, ny)[p])}
            self.second = {
                (p, i, j): copies.slot()
                for p in (0, 1)
                for i in range((nx, ny)[p])
                for j in range(1, (ny, nx)[p])
            }

        def source(self, part, i):
            if part == 0:
                return ty * nx + lax.rem(tx - i + nx, nx)
            return lax.rem(ty - i + ny, ny) * nx + tx

        def start(self, src):
            for p in (0, 1):
                for j in range(1, (nx, ny)[p]):
                    copies.send(self.first[p, j], src(p), self.at(t, p), (at_x, at_y)[p](j))
            for p in (0, 1):
                self.cross(p, 0, src(p))

        def cross(self, p, i, src):
            for j in range(1, (ny, nx)[p]):
                copies.send(
                    self.second[p, i, j], src, self.at(self.source(p, i), p), (at_y, at_x)[p](j)
                )

        def forward(self):
            for p in (0, 1):
                for i in range(1, (nx, ny)[p]):
                    block = self.at(self.source(p, i), p)
                    copies.receive(self.first[p, i], block, (at_x, at_y)[p](i))
                    self.cross(p, i, block)

        def finish(self):
            for p in (0, 1):
                for i in range((nx, ny)[p]):
                    for j in range(1, (ny, nx)[p]):
                        if p == 0:
                            came = lax.rem(ty - j + ny, ny) * nx + lax.rem(tx - i + nx, nx)
                        else:
                            came = lax.rem(ty - i + ny, ny) * nx + lax.rem(tx - j + nx, nx)
                        copies.receive(self.second[p, i, j], self.at(came, p), (at_y, at_x)[p](j))

    tokens = Plane(tok_at)
    half = rows // 2
    tokens.start(lambda p: hid_v.at[pl.ds(p * half, half), :])
    for way, device, has, sign in links:
        copies.send(line["o", way, 1], o_v, o_at(t, d), device, has)
    to_partner = {}
    for s in range(1 - nz, nz):
        to_partner["w", s] = copies.slot()
        to_partner["o", s] = copies.slot()
    copies.send(to_partner["w", 0], w_v, w_at(d), partner)
    stores = [
        pltpu.make_async_copy(w_v, w_at(d), local_sem.at[0]),
        pltpu.make_async_copy(hid_v, tok.at[pl.ds(pl.multiple_of(t * rows, 8), rows), :], local_sem.at[3]),
        pltpu.make_async_copy(o_v, o_at(t, d), local_sem.at[4]),
    ]
    for store in stores:
        store.start()

    def pass_on(name, place, s):
        for way, device, has, sign in links:
            here = (z >= s) if way == "up" else (z + s < nz)
            dp = jnp.clip(d - sign * s * CORES, 0, nz * CORES - 1)
            block = place(dp)
            copies.receive(line[name, way, s], block, device, here)
            if s + 1 < nz:
                copies.send(line[name, way, s + 1], block, block, device, here & has)
            if name == "w":
                copies.send(to_partner["w", sign * s], block, block, partner, here)

    def o_place(dp):
        return o_at(t, dp)

    planes = []

    def spread(step):
        dp = lax.rem(z + step, nz) * CORES + c
        plane = Plane(lambda tensor, p: o_at(tensor, dp, p))
        if step == 0:
            oh = o_rows // 2
            plane.start(lambda p: o_v.at[pl.ds(p * oh, oh), :])
        else:
            plane.start(lambda p: o_at(t, dp, p))
        planes.append((plane, dp))

    pass_on("w", w_at, 1)
    tokens.forward()
    spread(0)
    pass_on("o", o_place, 1)
    for s in range(2, nz):
        pass_on("w", w_at, s)
        pass_on("o", o_place, s)
    for store in stores:
        store.wait()
    for step in range(1, nz):
        spread(step)
    for plane, dp in planes:
        plane.forward()
    tokens.finish()
    column_slots = [copies.slot() for _ in planes]
    for slot, (plane, dp) in zip(column_slots, planes):
        plane.finish()
        column = full.at[dp]
        copies.send(slot, column, column, partner)

    copies.receive(to_partner["w", 0], w_at(z * CORES + 1 - c), partner)
    for s in range(1, nz):
        for way, device, has, sign in links:
            here = (z >= s) if way == "up" else (z + s < nz)
            dp = jnp.clip(z - sign * s, 0, nz - 1) * CORES + 1 - c
            copies.receive(to_partner["w", sign * s], w_at(dp), partner, here)
    for step, slot in enumerate(column_slots):
        dp = lax.rem(z + step, nz) * CORES + 1 - c
        column = full.at[dp]
        copies.receive(slot, column, partner)
    copies.finish()


def attend_kernel(
    plan, qkv, q_gain, k_gain, out, sums, q_bf, k_bf, v_bf, att, local_sem, send_sem, recv_sem
):
    tensor_size, heads_dev, kv_count, heads_all, k_share = plan
    t, d = lax.axis_index("tensor"), lax.axis_index("dp")
    q_width, kv_width = heads_dev * HD, kv_count * HD
    seq_len = qkv.shape[0]
    rows = seq_len // tensor_size
    copies = Copies(send_sem, recv_sem)

    def at(j):
        return {"tensor": lax.rem(t + j, tensor_size), "dp": d}

    barrier = pltpu.get_barrier_semaphore()
    for j in range(1, tensor_size):
        pl.semaphore_signal(barrier, inc=1, device_id=at(j), device_id_type=MESH)

    queries = qkv[:, :q_width]
    key_rows = qkv[:, q_width : q_width + kv_width]

    def row_sums(block):
        ones = jnp.ones((8, block.shape[1]), jnp.float32)
        return lax.dot_general(
            ones,
            block * block,
            (((1,), (1,)), ((), ())),
            precision=lax.Precision.HIGHEST,
            preferred_element_type=jnp.float32,
        )

    upper = lax.broadcasted_iota(jnp.int32, (8, seq_len), 0) < 4
    sums[0] = jnp.where(upper, row_sums(queries), row_sums(key_rows) * k_share)
    pl.semaphore_wait(barrier, tensor_size - 1)
    slots = [copies.slot() for _ in range(1, tensor_size)]
    for j in range(1, tensor_size):
        copies.send(slots[j - 1], sums.at[0], sums.at[j], at(j))
    v_bf[...] = qkv[:, q_width + kv_width :].astype(jnp.bfloat16)
    for j in range(1, tensor_size):
        copies.receive(slots[j - 1], sums.at[j], at(j))
    total = sums[0]
    for j in range(1, tensor_size):
        total = total + sums[j]

    def as_column(first):
        pick = (lax.broadcasted_iota(jnp.int32, (8, HD), 0) == first).astype(jnp.float32)
        return lax.dot_general(
            total,
            pick,
            (((0,), (0,)), ((), ())),
            precision=lax.Precision.HIGHEST,
            preferred_element_type=jnp.float32,
        )

    q_scale = lax.rsqrt(as_column(0) / (heads_all * HD) + epsilon)
    k_scale = lax.rsqrt(as_column(4) / (KV_HEADS * HD) + epsilon)
    for h in range(heads_dev):
        cols = slice(h * HD, (h + 1) * HD)
        q_bf[:, cols] = (qkv[:, cols] * q_scale * q_gain[:, cols]).astype(jnp.bfloat16)
    for g in range(kv_count):
        cols = slice(g * HD, (g + 1) * HD)
        source = slice(q_width + g * HD, q_width + (g + 1) * HD)
        k_bf[:, cols] = (qkv[:, source] * k_scale * k_gain[:, cols]).astype(jnp.bfloat16)

    def columns(tensor):
        return out.at[:, pl.ds(pl.multiple_of(tensor * q_width, HD), q_width)]

    back = [copies.slot() for _ in range(tensor_size)]
    for i in range(tensor_size):
        block, seen = slice(i * rows, (i + 1) * rows), (i + 1) * rows
        rows_idx = lax.broadcasted_iota(jnp.int32, (rows, seen), 0) + i * rows
        cols_idx = lax.broadcasted_iota(jnp.int32, (rows, seen), 1)
        for h in range(heads_dev):
            g = h * kv_count // heads_dev
            cols, kv_cols = slice(h * HD, (h + 1) * HD), slice(g * HD, (g + 1) * HD)
            scores = lax.dot_general(
                q_bf[block, cols],
                k_bf[:seen, kv_cols],
                (((1,), (1,)), ((), ())),
                preferred_element_type=jnp.float32,
            ) * HD ** (-0.5)
            scores = jnp.where(cols_idx <= rows_idx, scores, -1e30)
            expo = jnp.exp(scores - jnp.max(scores, axis=1, keepdims=True))
            weights = (expo * (1.0 / jnp.sum(expo, axis=1, keepdims=True))).astype(jnp.bfloat16)
            att[block, cols] = jnp.dot(
                weights, v_bf[:seen, kv_cols], preferred_element_type=jnp.float32
            ).astype(jnp.bfloat16)
        own = att.at[pl.ds(i * rows, rows), :]
        j = lax.rem(i - t + tensor_size, tensor_size)
        copy = pltpu.make_async_remote_copy(
            src_ref=own,
            dst_ref=columns(t),
            send_sem=send_sem.at[back[i]],
            recv_sem=recv_sem.at[back[0] + j],
            device_id={"tensor": i, "dp": d},
            device_id_type=MESH,
        )
        copies.sent.append((copy, t != i))
        pl.when(t != i)(copy.start)
    mine = pltpu.make_async_copy(
        att.at[pl.ds(pl.multiple_of(t * rows, 8), rows), :], columns(t), local_sem.at[0]
    )
    mine.start()
    mine.wait()
    for j in range(1, tensor_size):
        copies.receive(back[j], columns(lax.rem(t - j + tensor_size, tensor_size)), at(j))
    copies.finish()


def project_kernel(att, weight, hid, gain, out, projected, squares):
    n = pl.program_id(0)
    blocks, _, cols = projected.shape
    block = jnp.dot(att[...], weight[0], preferred_element_type=jnp.float32)
    projected[n] = block
    here = jnp.sum(block * block, axis=1, keepdims=True)

    @pl.when(n == 0)
    def _():
        squares[...] = here

    @pl.when(n > 0)
    def _():
        squares[...] += here

    @pl.when(n == blocks - 1)
    def _():
        scale = lax.rsqrt(squares[...] / (blocks * cols) + epsilon)
        for b in range(blocks):
            part = slice(b * cols, (b + 1) * cols)
            out[:, part] = (
                hid[:, part].astype(jnp.float32) + projected[b] * scale * gain[:, part]
            ).astype(out.dtype)


def local(hidden_in, q_weight, k_weight, v_weight, q_gain, k_gain, o_weight, post_gain):
    tensor_size, dp_size = lax.axis_size("tensor"), lax.axis_size("dp")
    heads_dev = q_weight.shape[1] // HD
    heads_all = heads_dev * tensor_size
    group_size = heads_all // KV_HEADS
    kv_count = max(1, heads_dev // group_size)
    kv_first = lax.axis_index("tensor") * heads_dev // group_size
    k_share = min(1.0, heads_dev / group_size)
    q_width, kv_width = heads_dev * HD, kv_count * HD
    width = q_width + 2 * kv_width
    rows, model = hidden_in.shape
    depth = q_weight.shape[0]
    o_rows, o_cols = o_weight.shape
    seq_len = rows * tensor_size
    ny, nx = plane_of(tensor_size)
    nz = dp_size // CORES
    any_space = pl.BlockSpec(memory_space=pl.ANY)
    vmem = pl.BlockSpec(memory_space=pltpu.VMEM)
    bf16 = jnp.bfloat16

    per_plane = (nx - 1) + (ny - 1) + nx * (ny - 1) + ny * (nx - 1)
    slots = 4 * (nz - 1) + (nz + 1) * per_plane + 2 * (2 * nz - 1) + nz
    tokens, weights, o_full = pl.pallas_call(
        functools.partial(
            gather_kernel, (ny, nx, nz, q_width, kv_width, heads_dev, group_size)
        ),
        out_shape=(
            jax.ShapeDtypeStruct((seq_len, model), bf16),
            jax.ShapeDtypeStruct((depth * dp_size, width), bf16),
            jax.ShapeDtypeStruct((dp_size, o_rows * tensor_size, o_cols), bf16),
        ),
        in_specs=[any_space] * 5,
        out_specs=(any_space,) * 3,
        scratch_shapes=[
            pltpu.VMEM((rows, model), bf16),
            pltpu.VMEM((depth, width), bf16),
            pltpu.VMEM((o_rows, o_cols), bf16),
            pltpu.SemaphoreType.DMA((5,)),
            pltpu.SemaphoreType.DMA((slots,)),
            pltpu.SemaphoreType.DMA((slots,)),
        ],
        compiler_params=pltpu.CompilerParams(collective_id=0, has_side_effects=True),
        name="gather",
    )(hidden_in, q_weight, k_weight, v_weight, o_weight)

    qkv = jnp.dot(tokens, weights, preferred_element_type=jnp.float32)
    k_gain_part = lax.dynamic_slice_in_dim(k_gain, kv_first * HD, kv_width, 0)
    attended = pl.pallas_call(
        functools.partial(attend_kernel, (tensor_size, heads_dev, kv_count, heads_all, k_share)),
        out_shape=jax.ShapeDtypeStruct((rows, q_width * tensor_size), bf16),
        in_specs=[vmem] * 3,
        out_specs=any_space,
        scratch_shapes=[
            pltpu.VMEM((tensor_size, 8, seq_len), jnp.float32),
            pltpu.VMEM((seq_len, q_width), bf16),
            pltpu.VMEM((seq_len, kv_width), bf16),
            pltpu.VMEM((seq_len, kv_width), bf16),
            pltpu.VMEM((seq_len, q_width), bf16),
            pltpu.SemaphoreType.DMA((1,)),
            pltpu.SemaphoreType.DMA((2 * tensor_size,)),
            pltpu.SemaphoreType.DMA((2 * tensor_size,)),
        ],
        compiler_params=pltpu.CompilerParams(collective_id=1, has_side_effects=True),
        name="attend",
    )(qkv, q_gain[None], k_gain_part[None])

    return pl.pallas_call(
        project_kernel,
        out_shape=jax.ShapeDtypeStruct((rows, model), bf16),
        grid=(dp_size,),
        in_specs=[
            pl.BlockSpec(attended.shape, lambda n: (0, 0)),
            pl.BlockSpec((1,) + o_full.shape[1:], lambda n: (n, 0, 0)),
            pl.BlockSpec((rows, model), lambda n: (0, 0)),
            pl.BlockSpec((1, model), lambda n: (0, 0)),
        ],
        out_specs=pl.BlockSpec((rows, model), lambda n: (0, 0)),
        scratch_shapes=[
            pltpu.VMEM((dp_size, rows, o_cols), jnp.float32),
            pltpu.VMEM((rows, 1), jnp.float32),
        ],
        name="project",
    )(attended, o_full, hidden_in, post_gain[None])


def solution(mesh):
    in_specs = (
        P(("dp", "tensor"), None),
        P("dp", "tensor"),
        P("dp", None),
        P("dp", None),
        P("tensor"),
        P(),
        P("tensor", "dp"),
        P(),
    )
    out_specs = P(("dp", "tensor"), None)
    return jax.shard_map(local, mesh=mesh, in_specs=in_specs, out_specs=out_specs, check_vma=False)
```

```python
import functools

import jax
import jax.numpy as jnp
from jax import lax
from jax.experimental import pallas as pl
from jax.experimental.pallas import tpu as pltpu
from jax.sharding import PartitionSpec as P

HD = 128
KV_HEADS = 8
CORES = 2
MESH = pl.DeviceIdType.MESH

epsilon = 1e-06


def plane_of(tensor_size):
    ny = max(n for n in range(1, tensor_size + 1) if tensor_size % n == 0 and n * n <= tensor_size)
    return ny, tensor_size // ny


class Copies:
    def __init__(self, send_sem, recv_sem):
        self.send_sem, self.recv_sem, self.count, self.sent = send_sem, recv_sem, 0, []

    def slot(self):
        self.count += 1
        return self.count - 1

    def make(self, slot, src, dst, device):
        return pltpu.make_async_remote_copy(
            src_ref=src,
            dst_ref=dst,
            send_sem=self.send_sem.at[slot],
            recv_sem=self.recv_sem.at[slot],
            device_id=device,
            device_id_type=MESH,
        )

    def send(self, slot, src, dst, device, when=None):
        copy = self.make(slot, src, dst, device)
        self.sent.append((copy, when))
        run(when, copy.start)

    def receive(self, slot, dst, device, when=None):
        run(when, self.make(slot, dst, dst, device).wait_recv)

    def finish(self):
        for copy, when in self.sent:
            run(when, copy.wait_send)


def run(when, action):
    if when is None:
        action()
    else:
        pl.when(when)(action)


def layer_kernel(
    plan,
    hid,
    qw,
    kw,
    vw,
    ow,
    q_gain,
    k_gain,
    full,
    out,
    tok,
    wts,
    o_v,
    qkv,
    sums,
    q_bf,
    k_bf,
    v_bf,
    att,
    local_sem,
    send_sem,
    recv_sem,
):
    ny, nx, nz, heads_dev, kv_count, group, k_share = plan
    q_width, kv_width = heads_dev * HD, kv_count * HD
    tensor_size = ny * nx
    t, d = lax.axis_index("tensor"), lax.axis_index("dp")
    tx, ty = lax.rem(t, nx), lax.div(t, nx)
    c, z = lax.rem(d, CORES), lax.div(d, CORES)
    rows, depth = hid.shape[0], qw.shape[0]
    o_rows, o_cols = ow.shape
    copies = Copies(send_sem, recv_sem)

    def at_x(j):
        return {"tensor": ty * nx + lax.rem(tx + j, nx), "dp": d}

    def at_y(j):
        return {"tensor": lax.rem(ty + j, ny) * nx + tx, "dp": d}

    up = {"tensor": t, "dp": jnp.minimum(d + CORES, nz * CORES - 1)}
    down = {"tensor": t, "dp": jnp.maximum(d - CORES, 0)}
    partner = {"tensor": t, "dp": z * CORES + 1 - c}
    has_up, has_down = z + 1 < nz, z > 0

    kv_first = pl.multiple_of(lax.div(t * heads_dev, group) * HD, HD)
    w_rows = pl.ds(pl.multiple_of(d * depth, 8), depth)
    loads = [
        pltpu.make_async_copy(qw, wts.at[w_rows, pl.ds(0, q_width)], local_sem.at[0]),
        pltpu.make_async_copy(
            kw.at[:, pl.ds(kv_first, kv_width)],
            wts.at[w_rows, pl.ds(q_width, kv_width)],
            local_sem.at[1],
        ),
        pltpu.make_async_copy(
            vw.at[:, pl.ds(kv_first, kv_width)],
            wts.at[w_rows, pl.ds(q_width + kv_width, kv_width)],
            local_sem.at[2],
        ),
        pltpu.make_async_copy(
            hid, tok.at[pl.ds(pl.multiple_of(t * rows, 8), rows), :], local_sem.at[3]
        ),
        pltpu.make_async_copy(ow, o_v, local_sem.at[4]),
    ]
    for load in loads:
        load.start()

    barrier = pltpu.get_barrier_semaphore()

    def greet(device):
        pl.semaphore_signal(barrier, inc=1, device_id=device, device_id_type=MESH)

    for j in range(1, tensor_size):
        greet({"tensor": lax.rem(t + j, tensor_size), "dp": d})
    greet(partner)
    run(has_up, lambda: greet(up))
    run(has_down, lambda: greet(down))
    pl.semaphore_wait(
        barrier, tensor_size + has_up.astype(jnp.int32) + has_down.astype(jnp.int32)
    )

    def w_at(dp):
        return wts.at[pl.ds(pl.multiple_of(dp * depth, 8), depth), :]

    def o_at(tensor, dp, part=None):
        size = o_rows if part is None else o_rows // 2
        start = tensor * o_rows + (0 if part is None else part * size)
        return full.at[dp, pl.ds(pl.multiple_of(start, 8), size), :]

    def tok_at(tensor, part):
        size = rows // 2
        return tok.at[pl.ds(pl.multiple_of(tensor * rows + part * size, 8), size), :]

    for load in loads:
        load.wait()
    line = {}
    for name in ("w", "o"):
        for way in ("up", "down"):
            for s in range(1, nz):
                line[name, way, s] = copies.slot()
    links = (("up", up, has_up, 1), ("down", down, has_down, -1))
    for way, device, has, sign in links:
        copies.send(line["w", way, 1], w_at(d), w_at(d), device, has)

    class Plane:
        def __init__(self, at):
            self.at = at
            self.first = {(p, j): copies.slot() for p in (0, 1) for j in range(1, (nx, ny)[p])}
            self.second = {
                (p, i, j): copies.slot()
                for p in (0, 1)
                for i in range((nx, ny)[p])
                for j in range(1, (ny, nx)[p])
            }

        def source(self, part, i):
            if part == 0:
                return ty * nx + lax.rem(tx - i + nx, nx)
            return lax.rem(ty - i + ny, ny) * nx + tx

        def start(self, src):
            for p in (0, 1):
                for j in range(1, (nx, ny)[p]):
                    copies.send(self.first[p, j], src(p), self.at(t, p), (at_x, at_y)[p](j))
            for p in (0, 1):
                self.cross(p, 0, src(p))

        def cross(self, p, i, src):
            for j in range(1, (ny, nx)[p]):
                copies.send(
                    self.second[p, i, j], src, self.at(self.source(p, i), p), (at_y, at_x)[p](j)
                )

        def forward(self):
            for p in (0, 1):
                for i in range(1, (nx, ny)[p]):
                    block = self.at(self.source(p, i), p)
                    copies.receive(self.first[p, i], block, (at_x, at_y)[p](i))
                    self.cross(p, i, block)

        def finish(self):
            for p in (0, 1):
                for i in range((nx, ny)[p]):
                    for j in range(1, (ny, nx)[p]):
                        if p == 0:
                            came = lax.rem(ty - j + ny, ny) * nx + lax.rem(tx - i + nx, nx)
                        else:
                            came = lax.rem(ty - i + ny, ny) * nx + lax.rem(tx - j + nx, nx)
                        copies.receive(self.second[p, i, j], self.at(came, p), (at_y, at_x)[p](j))

    tokens = Plane(tok_at)
    tokens.start(lambda p: tok_at(t, p))
    for way, device, has, sign in links:
        copies.send(line["o", way, 1], o_v, o_at(t, d), device, has)
    to_partner = {}
    for s in range(1 - nz, nz):
        to_partner["w", s] = copies.slot()
        to_partner["o", s] = copies.slot()
    copies.send(to_partner["w", 0], w_at(d), w_at(d), partner)
    store = pltpu.make_async_copy(o_v, o_at(t, d), local_sem.at[4])
    store.start()

    def pass_on(name, place, s):
        for way, device, has, sign in links:
            here = (z >= s) if way == "up" else (z + s < nz)
            dp = jnp.clip(d - sign * s * CORES, 0, nz * CORES - 1)
            block = place(dp)
            copies.receive(line[name, way, s], block, device, here)
            if s + 1 < nz:
                copies.send(line[name, way, s + 1], block, block, device, here & has)
            if name == "w":
                copies.send(to_partner["w", sign * s], block, block, partner, here)

    def o_place(dp):
        return o_at(t, dp)

    planes = []

    def spread(step):
        dp = lax.rem(z + step, nz) * CORES + c
        plane = Plane(lambda tensor, p: o_at(tensor, dp, p))
        if step == 0:
            oh = o_rows // 2
            plane.start(lambda p: o_v.at[pl.ds(p * oh, oh), :])
        else:
            plane.start(lambda p: o_at(t, dp, p))
        planes.append((plane, dp))

    pass_on("w", w_at, 1)
    tokens.forward()
    spread(0)
    pass_on("o", o_place, 1)
    for s in range(2, nz):
        pass_on("w", w_at, s)
        pass_on("o", o_place, s)
    store.wait()
    for step in range(1, nz):
        spread(step)
    copies.receive(to_partner["w", 0], w_at(z * CORES + 1 - c), partner)
    for s in range(1, nz):
        for way, device, has, sign in links:
            here = (z >= s) if way == "up" else (z + s < nz)
            dp = jnp.clip(z - sign * s, 0, nz - 1) * CORES + 1 - c
            copies.receive(to_partner["w", sign * s], w_at(dp), partner, here)

    width = wts.shape[1]
    step_cols = 2 * HD if width % (2 * HD) == 0 else HD

    def multiply(tensor):
        block = pl.ds(pl.multiple_of(tensor * rows, 8), rows)

        def one(n, carry):
            cols = pl.ds(pl.multiple_of(n * step_cols, HD), step_cols)
            qkv[block, cols] = jnp.dot(
                tok[block, :], wts[:, cols], preferred_element_type=jnp.float32
            )
            return carry

        lax.fori_loop(0, width // step_cols, one, 0)

    multiply(t)
    tokens.finish()

    def others(j, carry):
        multiply(lax.rem(t + j, tensor_size))
        return carry

    lax.fori_loop(1, tensor_size, others, 0)
    for plane, dp in planes:
        plane.forward()
    attend(
        (tensor_size, heads_dev, kv_count, heads_dev * tensor_size, k_share),
        copies,
        qkv,
        q_gain,
        k_gain,
        kv_first,
        out,
        sums,
        q_bf,
        k_bf,
        v_bf,
        att,
        local_sem,
    )
    column_slots = [copies.slot() for _ in planes]
    for slot, (plane, dp) in zip(column_slots, planes):
        plane.finish()
        copies.send(slot, full.at[dp], full.at[dp], partner)
    for step, slot in enumerate(column_slots):
        dp = lax.rem(z + step, nz) * CORES + 1 - c
        copies.receive(slot, full.at[dp], partner)
    copies.finish()


def attend(
    plan, copies, qkv, q_gain, k_gain, kv_first, out, sums, q_bf, k_bf, v_bf, att, local_sem
):
    tensor_size, heads_dev, kv_count, heads_all, k_share = plan
    t, d = lax.axis_index("tensor"), lax.axis_index("dp")
    q_width, kv_width = heads_dev * HD, kv_count * HD
    seq_len = qkv.shape[0]
    rows = seq_len // tensor_size
    send_sem, recv_sem = copies.send_sem, copies.recv_sem

    def at(j):
        return {"tensor": lax.rem(t + j, tensor_size), "dp": d}

    queries = qkv[:, :q_width]
    key_rows = qkv[:, q_width : q_width + kv_width]

    def row_sums(block):
        ones = jnp.ones((8, block.shape[1]), jnp.float32)
        return lax.dot_general(
            ones,
            block * block,
            (((1,), (1,)), ((), ())),
            precision=lax.Precision.HIGHEST,
            preferred_element_type=jnp.float32,
        )

    upper = lax.broadcasted_iota(jnp.int32, (8, seq_len), 0) < 4
    sums[0] = jnp.where(upper, row_sums(queries), row_sums(key_rows) * k_share)
    slots = [copies.slot() for _ in range(1, tensor_size)]
    for j in range(1, tensor_size):
        copies.send(slots[j - 1], sums.at[0], sums.at[j], at(j))
    v_bf[...] = qkv[:, q_width + kv_width :].astype(jnp.bfloat16)
    for j in range(1, tensor_size):
        copies.receive(slots[j - 1], sums.at[j], at(j))
    total = sums[0]
    for j in range(1, tensor_size):
        total = total + sums[j]

    def as_column(first):
        pick = (lax.broadcasted_iota(jnp.int32, (8, HD), 0) == first).astype(jnp.float32)
        return lax.dot_general(
            total,
            pick,
            (((0,), (0,)), ((), ())),
            precision=lax.Precision.HIGHEST,
            preferred_element_type=jnp.float32,
        )

    q_scale = lax.rsqrt(as_column(0) / (heads_all * HD) + epsilon)
    k_scale = lax.rsqrt(as_column(4) / (KV_HEADS * HD) + epsilon)
    for h in range(heads_dev):
        cols = slice(h * HD, (h + 1) * HD)
        q_bf[:, cols] = (qkv[:, cols] * q_scale * q_gain[:, cols]).astype(jnp.bfloat16)
    for g in range(kv_count):
        cols = slice(g * HD, (g + 1) * HD)
        gain = k_gain[:, pl.ds(pl.multiple_of(kv_first + g * HD, HD), HD)]
        source = slice(q_width + g * HD, q_width + (g + 1) * HD)
        k_bf[:, cols] = (qkv[:, source] * k_scale * gain).astype(jnp.bfloat16)

    def columns(tensor):
        return out.at[:, pl.ds(pl.multiple_of(tensor * q_width, HD), q_width)]

    back = [copies.slot() for _ in range(tensor_size)]
    for i in range(tensor_size):
        block, seen = slice(i * rows, (i + 1) * rows), (i + 1) * rows
        rows_idx = lax.broadcasted_iota(jnp.int32, (rows, seen), 0) + i * rows
        cols_idx = lax.broadcasted_iota(jnp.int32, (rows, seen), 1)
        for h in range(heads_dev):
            g = h * kv_count // heads_dev
            cols, kv_cols = slice(h * HD, (h + 1) * HD), slice(g * HD, (g + 1) * HD)
            scores = lax.dot_general(
                q_bf[block, cols],
                k_bf[:seen, kv_cols],
                (((1,), (1,)), ((), ())),
                preferred_element_type=jnp.float32,
            ) * HD ** (-0.5)
            scores = jnp.where(cols_idx <= rows_idx, scores, -1e30)
            expo = jnp.exp(scores - jnp.max(scores, axis=1, keepdims=True))
            weights = (expo * (1.0 / jnp.sum(expo, axis=1, keepdims=True))).astype(jnp.bfloat16)
            att[block, cols] = jnp.dot(
                weights, v_bf[:seen, kv_cols], preferred_element_type=jnp.float32
            ).astype(jnp.bfloat16)
        own = att.at[pl.ds(i * rows, rows), :]
        j = lax.rem(i - t + tensor_size, tensor_size)
        copy = pltpu.make_async_remote_copy(
            src_ref=own,
            dst_ref=columns(t),
            send_sem=send_sem.at[back[i]],
            recv_sem=recv_sem.at[back[0] + j],
            device_id={"tensor": i, "dp": d},
            device_id_type=MESH,
        )
        copies.sent.append((copy, t != i))
        pl.when(t != i)(copy.start)
    mine = pltpu.make_async_copy(
        att.at[pl.ds(pl.multiple_of(t * rows, 8), rows), :], columns(t), local_sem.at[0]
    )
    mine.start()
    mine.wait()
    for j in range(1, tensor_size):
        copies.receive(back[j], columns(lax.rem(t - j + tensor_size, tensor_size)), at(j))


def project_kernel(att, weight, hid, gain, out, projected, squares):
    n = pl.program_id(0)
    blocks, _, cols = projected.shape
    block = jnp.dot(att[...], weight[0], preferred_element_type=jnp.float32)
    projected[n] = block
    here = jnp.sum(block * block, axis=1, keepdims=True)

    @pl.when(n == 0)
    def _():
        squares[...] = here

    @pl.when(n > 0)
    def _():
        squares[...] += here

    @pl.when(n == blocks - 1)
    def _():
        scale = lax.rsqrt(squares[...] / (blocks * cols) + epsilon)
        for b in range(blocks):
            part = slice(b * cols, (b + 1) * cols)
            out[:, part] = (
                hid[:, part].astype(jnp.float32) + projected[b] * scale * gain[:, part]
            ).astype(out.dtype)


def local(hidden_in, q_weight, k_weight, v_weight, q_gain, k_gain, o_weight, post_gain):
    tensor_size, dp_size = lax.axis_size("tensor"), lax.axis_size("dp")
    heads_dev = q_weight.shape[1] // HD
    heads_all = heads_dev * tensor_size
    group_size = heads_all // KV_HEADS
    kv_count = max(1, heads_dev // group_size)
    k_share = min(1.0, heads_dev / group_size)
    q_width, kv_width = heads_dev * HD, kv_count * HD
    width = q_width + 2 * kv_width
    rows, model = hidden_in.shape
    depth = q_weight.shape[0]
    o_rows, o_cols = o_weight.shape
    seq_len = rows * tensor_size
    ny, nx = plane_of(tensor_size)
    nz = dp_size // CORES
    any_space = pl.BlockSpec(memory_space=pl.ANY)
    vmem = pl.BlockSpec(memory_space=pltpu.VMEM)
    bf16 = jnp.bfloat16

    per_plane = (nx - 1) + (ny - 1) + nx * (ny - 1) + ny * (nx - 1)
    slots = 4 * (nz - 1) + (nz + 1) * per_plane + 2 * (2 * nz - 1) + nz + 2 * tensor_size
    o_full, attended = pl.pallas_call(
        functools.partial(
            layer_kernel, (ny, nx, nz, heads_dev, kv_count, group_size, k_share)
        ),
        out_shape=(
            jax.ShapeDtypeStruct((dp_size, o_rows * tensor_size, o_cols), bf16),
            jax.ShapeDtypeStruct((rows, q_width * tensor_size), bf16),
        ),
        in_specs=[any_space] * 5 + [vmem] * 2,
        out_specs=(any_space,) * 2,
        scratch_shapes=[
            pltpu.VMEM((seq_len, model), bf16),
            pltpu.VMEM((depth * dp_size, width), bf16),
            pltpu.VMEM((o_rows, o_cols), bf16),
            pltpu.VMEM((seq_len, width), jnp.float32),
            pltpu.VMEM((tensor_size, 8, seq_len), jnp.float32),
            pltpu.VMEM((seq_len, q_width), bf16),
            pltpu.VMEM((seq_len, kv_width), bf16),
            pltpu.VMEM((seq_len, kv_width), bf16),
            pltpu.VMEM((seq_len, q_width), bf16),
            pltpu.SemaphoreType.DMA((5,)),
            pltpu.SemaphoreType.DMA((slots,)),
            pltpu.SemaphoreType.DMA((slots,)),
        ],
        compiler_params=pltpu.CompilerParams(collective_id=0, has_side_effects=True),
        name="layer",
    )(hidden_in, q_weight, k_weight, v_weight, o_weight, q_gain[None], k_gain[None])

    return pl.pallas_call(
        project_kernel,
        out_shape=jax.ShapeDtypeStruct((rows, model), bf16),
        grid=(dp_size,),
        in_specs=[
            pl.BlockSpec(attended.shape, lambda n: (0, 0)),
            pl.BlockSpec((1,) + o_full.shape[1:], lambda n: (n, 0, 0)),
            pl.BlockSpec((rows, model), lambda n: (0, 0)),
            pl.BlockSpec((1, model), lambda n: (0, 0)),
        ],
        out_specs=pl.BlockSpec((rows, model), lambda n: (0, 0)),
        scratch_shapes=[
            pltpu.VMEM((dp_size, rows, o_cols), jnp.float32),
            pltpu.VMEM((rows, 1), jnp.float32),
        ],
        name="project",
    )(attended, o_full, hidden_in, post_gain[None])


def solution(mesh):
    in_specs = (
        P(("dp", "tensor"), None),
        P("dp", "tensor"),
        P("dp", None),
        P("dp", None),
        P("tensor"),
        P(),
        P("tensor", "dp"),
        P(),
    )
    out_specs = P(("dp", "tensor"), None)
    return jax.shard_map(local, mesh=mesh, in_specs=in_specs, out_specs=out_specs, check_vma=False)
```

```python
import functools

import jax
import jax.numpy as jnp
from jax import lax
from jax.experimental import pallas as pl
from jax.experimental.pallas import tpu as pltpu
from jax.sharding import PartitionSpec as P

HD = 128
KV_HEADS = 8
CORES = 2
MESH = pl.DeviceIdType.MESH

epsilon = 1e-06


def plane_of(tensor_size):
    ny = max(n for n in range(1, tensor_size + 1) if tensor_size % n == 0 and n * n <= tensor_size)
    return ny, tensor_size // ny


class Copies:
    def __init__(self, send_sem, recv_sem):
        self.send_sem, self.recv_sem, self.count, self.sent = send_sem, recv_sem, 0, []

    def slot(self):
        self.count += 1
        return self.count - 1

    def make(self, slot, src, dst, device):
        return pltpu.make_async_remote_copy(
            src_ref=src,
            dst_ref=dst,
            send_sem=self.send_sem.at[slot],
            recv_sem=self.recv_sem.at[slot],
            device_id=device,
            device_id_type=MESH,
        )

    def send(self, slot, src, dst, device, when=None):
        copy = self.make(slot, src, dst, device)
        self.sent.append((copy, when))
        run(when, copy.start)

    def receive(self, slot, dst, device, when=None):
        run(when, self.make(slot, dst, dst, device).wait_recv)

    def finish(self):
        for copy, when in self.sent:
            run(when, copy.wait_send)


def run(when, action):
    if when is None:
        action()
    else:
        pl.when(when)(action)


def layer_kernel(
    plan,
    hid,
    qw,
    kw,
    vw,
    ow,
    q_gain,
    k_gain,
    full,
    out,
    tok,
    wts,
    o_v,
    qkv,
    sums,
    q_bf,
    k_bf,
    v_bf,
    att,
    local_sem,
    send_sem,
    recv_sem,
):
    ny, nx, nz, heads_dev, kv_count, group, k_share = plan
    q_width, kv_width = heads_dev * HD, kv_count * HD
    tensor_size = ny * nx
    t, d = lax.axis_index("tensor"), lax.axis_index("dp")
    tx, ty = lax.rem(t, nx), lax.div(t, nx)
    c, z = lax.rem(d, CORES), lax.div(d, CORES)
    rows, depth = hid.shape[0], qw.shape[0]
    o_rows, o_cols = ow.shape
    copies = Copies(send_sem, recv_sem)

    def at_x(j):
        return {"tensor": ty * nx + lax.rem(tx + j, nx), "dp": d}

    def at_y(j):
        return {"tensor": lax.rem(ty + j, ny) * nx + tx, "dp": d}

    up = {"tensor": t, "dp": jnp.minimum(d + CORES, nz * CORES - 1)}
    down = {"tensor": t, "dp": jnp.maximum(d - CORES, 0)}
    partner = {"tensor": t, "dp": z * CORES + 1 - c}
    has_up, has_down = z + 1 < nz, z > 0

    kv_first = pl.multiple_of(lax.div(t * heads_dev, group) * HD, HD)
    w_rows = pl.ds(pl.multiple_of(d * depth, 8), depth)
    loads = [
        pltpu.make_async_copy(qw, wts.at[w_rows, pl.ds(0, q_width)], local_sem.at[0]),
        pltpu.make_async_copy(
            kw.at[:, pl.ds(kv_first, kv_width)],
            wts.at[w_rows, pl.ds(q_width, kv_width)],
            local_sem.at[1],
        ),
        pltpu.make_async_copy(
            vw.at[:, pl.ds(kv_first, kv_width)],
            wts.at[w_rows, pl.ds(q_width + kv_width, kv_width)],
            local_sem.at[2],
        ),
        pltpu.make_async_copy(
            hid, tok.at[pl.ds(pl.multiple_of(t * rows, 8), rows), :], local_sem.at[3]
        ),
        pltpu.make_async_copy(ow, o_v, local_sem.at[4]),
    ]
    for load in loads:
        load.start()

    barrier = pltpu.get_barrier_semaphore()

    def greet(device):
        pl.semaphore_signal(barrier, inc=1, device_id=device, device_id_type=MESH)

    for j in range(1, tensor_size):
        greet({"tensor": lax.rem(t + j, tensor_size), "dp": d})
    greet(partner)
    run(has_up, lambda: greet(up))
    run(has_down, lambda: greet(down))
    pl.semaphore_wait(
        barrier, tensor_size + has_up.astype(jnp.int32) + has_down.astype(jnp.int32)
    )

    def w_at(dp):
        return wts.at[pl.ds(pl.multiple_of(dp * depth, 8), depth), :]

    def o_at(tensor, dp, part=None):
        size = o_rows if part is None else o_rows // 2
        start = tensor * o_rows + (0 if part is None else part * size)
        return full.at[dp, pl.ds(pl.multiple_of(start, 8), size), :]

    def tok_at(tensor, part):
        size = rows // 2
        return tok.at[pl.ds(pl.multiple_of(tensor * rows + part * size, 8), size), :]

    for load in loads:
        load.wait()
    line = {}
    for name in ("w", "o"):
        for way in ("up", "down"):
            for s in range(1, nz):
                line[name, way, s] = copies.slot()
    links = (("up", up, has_up, 1), ("down", down, has_down, -1))
    for way, device, has, sign in links:
        copies.send(line["w", way, 1], w_at(d), w_at(d), device, has)

    class Plane:
        def __init__(self, at, when=None):
            self.at, self.when = at, when
            self.first = {(p, j): copies.slot() for p in (0, 1) for j in range(1, (nx, ny)[p])}
            self.second = {
                (p, i, j): copies.slot()
                for p in (0, 1)
                for i in range((nx, ny)[p])
                for j in range(1, (ny, nx)[p])
            }

        def source(self, part, i):
            if part == 0:
                return ty * nx + lax.rem(tx - i + nx, nx)
            return lax.rem(ty - i + ny, ny) * nx + tx

        def start(self, src):
            for p in (0, 1):
                for j in range(1, (nx, ny)[p]):
                    copies.send(
                        self.first[p, j], src(p), self.at(t, p), (at_x, at_y)[p](j), self.when
                    )
            for p in (0, 1):
                self.cross(p, 0, src(p))

        def cross(self, p, i, src):
            for j in range(1, (ny, nx)[p]):
                copies.send(
                    self.second[p, i, j],
                    src,
                    self.at(self.source(p, i), p),
                    (at_y, at_x)[p](j),
                    self.when,
                )

        def forward(self):
            for p in (0, 1):
                for i in range(1, (nx, ny)[p]):
                    block = self.at(self.source(p, i), p)
                    copies.receive(self.first[p, i], block, (at_x, at_y)[p](i), self.when)
                    self.cross(p, i, block)

        def finish(self, diagonal=None):
            for p in (0, 1):
                for i in range((nx, ny)[p]):
                    for j in range(1, (ny, nx)[p]):
                        if diagonal is not None and diagonal != (i > 0):
                            continue
                        jx, jy = (i, j) if p == 0 else (j, i)
                        copies.receive(
                            self.second[p, i, j], self.at(near(jx, jy), p), (at_y, at_x)[p](j), self.when
                        )

    def near(jx, jy):
        return lax.rem(ty - jy + ny, ny) * nx + lax.rem(tx - jx + nx, nx)

    tokens = Plane(tok_at)
    tokens.start(lambda p: tok_at(t, p))
    to_partner = {("w", s): copies.slot() for s in range(1 - nz, nz)}
    copies.send(to_partner["w", 0], w_at(d), w_at(d), partner)
    store = pltpu.make_async_copy(o_v, o_at(t, d), local_sem.at[4])
    store.start()

    def pass_on(name, place, s):
        for way, device, has, sign in links:
            here = (z >= s) if way == "up" else (z + s < nz)
            dp = jnp.clip(d - sign * s * CORES, 0, nz * CORES - 1)
            block = place(dp)
            copies.receive(line[name, way, s], block, device, here)
            if s + 1 < nz:
                copies.send(line[name, way, s + 1], block, block, device, here & has)
            if name == "w":
                copies.send(to_partner["w", sign * s], block, block, partner, here)

    def o_place(dp):
        return o_at(t, dp)

    groups = [[] for _ in range(nz)]

    def spread(step, way=None):
        sign = -1 if way == "down" else 1
        dp = jnp.clip(d - sign * step * CORES, 0, nz * CORES - 1)
        when = None if step == 0 else (z >= step) if way == "up" else (z + step < nz)
        plane = Plane(lambda tensor, p: o_at(tensor, dp, p), when)
        half = o_rows // 2
        if step == 0:
            plane.start(lambda p: o_v.at[pl.ds(p * half, half), :])
        else:
            plane.start(lambda p: o_at(t, dp, p))
        groups[step].append((plane, sign * step))

    for s in range(1, nz):
        if s == nz - 1:
            for way, device, has, sign in links:
                copies.send(line["o", way, 1], o_v, o_at(t, d), device, has)
        pass_on("w", w_at, s)
        if s == 1:
            tokens.forward()
            spread(0)
    store.wait()
    copies.receive(to_partner["w", 0], w_at(z * CORES + 1 - c), partner)
    for s in range(1, nz):
        for way, device, has, sign in links:
            here = (z >= s) if way == "up" else (z + s < nz)
            dp = jnp.clip(z - sign * s, 0, nz - 1) * CORES + 1 - c
            copies.receive(to_partner["w", sign * s], w_at(dp), partner, here)

    width = wts.shape[1]
    step_cols = 2 * HD if width % (2 * HD) == 0 else HD

    def multiply(tensor):
        block = pl.ds(pl.multiple_of(tensor * rows, 8), rows)

        def one(n, carry):
            cols = pl.ds(pl.multiple_of(n * step_cols, HD), step_cols)
            qkv[block, cols] = jnp.dot(
                tok[block, :], wts[:, cols], preferred_element_type=jnp.float32
            )
            return carry

        lax.fori_loop(0, width // step_cols, one, 0)

    multiply(t)
    tokens.finish(diagonal=False)
    for jx in range(1, nx):
        multiply(near(jx, 0))
    for jy in range(1, ny):
        multiply(near(0, jy))
    for s in range(1, nz):
        pass_on("o", o_place, s)
        for way, *_ in links:
            spread(s, way)
    tokens.finish(diagonal=True)
    for jx in range(1, nx):
        for jy in range(1, ny):
            multiply(near(jx, jy))

    def between(i):
        for s in range(nz):
            if i == (tensor_size if s == nz - 1 else s * tensor_size // nz):
                for plane, _ in groups[s]:
                    plane.forward()

    attend(
        (tensor_size, heads_dev, kv_count, heads_dev * tensor_size, k_share),
        copies,
        between,
        qkv,
        q_gain,
        k_gain,
        kv_first,
        out,
        sums,
        q_bf,
        k_bf,
        v_bf,
        att,
        local_sem,
    )
    column_slots = {}
    for group in groups:
        for plane, step in group:
            plane.finish()
            column_slots[step] = copies.slot()
            column = full.at[jnp.clip(d - step * CORES, 0, nz * CORES - 1)]
            copies.send(column_slots[step], column, column, partner, plane.when)
    for group in groups:
        for plane, step in group:
            column = full.at[jnp.clip(z - step, 0, nz - 1) * CORES + 1 - c]
            copies.receive(column_slots[step], column, partner, plane.when)
    copies.finish()


def attend(
    plan, copies, between, qkv, q_gain, k_gain, kv_first, out, sums, q_bf, k_bf, v_bf, att, local_sem
):
    tensor_size, heads_dev, kv_count, heads_all, k_share = plan
    t, d = lax.axis_index("tensor"), lax.axis_index("dp")
    q_width, kv_width = heads_dev * HD, kv_count * HD
    seq_len = qkv.shape[0]
    rows = seq_len // tensor_size
    send_sem, recv_sem = copies.send_sem, copies.recv_sem

    def at(j):
        return {"tensor": lax.rem(t + j, tensor_size), "dp": d}

    queries = qkv[:, :q_width]
    key_rows = qkv[:, q_width : q_width + kv_width]

    def row_sums(block):
        ones = jnp.ones((8, block.shape[1]), jnp.float32)
        return lax.dot_general(
            ones,
            block * block,
            (((1,), (1,)), ((), ())),
            precision=lax.Precision.HIGHEST,
            preferred_element_type=jnp.float32,
        )

    upper = lax.broadcasted_iota(jnp.int32, (8, seq_len), 0) < 4
    sums[0] = jnp.where(upper, row_sums(queries), row_sums(key_rows) * k_share)
    slots = [copies.slot() for _ in range(1, tensor_size)]
    for j in range(1, tensor_size):
        copies.send(slots[j - 1], sums.at[0], sums.at[j], at(j))
    v_bf[...] = qkv[:, q_width + kv_width :].astype(jnp.bfloat16)
    for j in range(1, tensor_size):
        copies.receive(slots[j - 1], sums.at[j], at(j))
    total = sums[0]
    for j in range(1, tensor_size):
        total = total + sums[j]

    def as_column(first):
        pick = (lax.broadcasted_iota(jnp.int32, (8, HD), 0) == first).astype(jnp.float32)
        return lax.dot_general(
            total,
            pick,
            (((0,), (0,)), ((), ())),
            precision=lax.Precision.HIGHEST,
            preferred_element_type=jnp.float32,
        )

    q_scale = lax.rsqrt(as_column(0) / (heads_all * HD) + epsilon)
    k_scale = lax.rsqrt(as_column(4) / (KV_HEADS * HD) + epsilon)
    for h in range(heads_dev):
        cols = slice(h * HD, (h + 1) * HD)
        q_bf[:, cols] = (qkv[:, cols] * q_scale * q_gain[:, cols]).astype(jnp.bfloat16)
    for g in range(kv_count):
        cols = slice(g * HD, (g + 1) * HD)
        gain = k_gain[:, pl.ds(pl.multiple_of(kv_first + g * HD, HD), HD)]
        source = slice(q_width + g * HD, q_width + (g + 1) * HD)
        k_bf[:, cols] = (qkv[:, source] * k_scale * gain).astype(jnp.bfloat16)

    def columns(tensor):
        return out.at[:, pl.ds(pl.multiple_of(tensor * q_width, HD), q_width)]

    back = [copies.slot() for _ in range(tensor_size)]
    for i in range(tensor_size):
        between(i)
        block, seen = slice(i * rows, (i + 1) * rows), (i + 1) * rows
        rows_idx = lax.broadcasted_iota(jnp.int32, (rows, seen), 0) + i * rows
        cols_idx = lax.broadcasted_iota(jnp.int32, (rows, seen), 1)
        for h in range(heads_dev):
            g = h * kv_count // heads_dev
            cols, kv_cols = slice(h * HD, (h + 1) * HD), slice(g * HD, (g + 1) * HD)
            scores = lax.dot_general(
                q_bf[block, cols],
                k_bf[:seen, kv_cols],
                (((1,), (1,)), ((), ())),
                preferred_element_type=jnp.float32,
            ) * HD ** (-0.5)
            scores = jnp.where(cols_idx <= rows_idx, scores, -1e30)
            expo = jnp.exp(scores - jnp.max(scores, axis=1, keepdims=True))
            weights = (expo * (1.0 / jnp.sum(expo, axis=1, keepdims=True))).astype(jnp.bfloat16)
            att[block, cols] = jnp.dot(
                weights, v_bf[:seen, kv_cols], preferred_element_type=jnp.float32
            ).astype(jnp.bfloat16)
        own = att.at[pl.ds(i * rows, rows), :]
        j = lax.rem(i - t + tensor_size, tensor_size)
        copy = pltpu.make_async_remote_copy(
            src_ref=own,
            dst_ref=columns(t),
            send_sem=send_sem.at[back[i]],
            recv_sem=recv_sem.at[back[0] + j],
            device_id={"tensor": i, "dp": d},
            device_id_type=MESH,
        )
        copies.sent.append((copy, t != i))
        pl.when(t != i)(copy.start)
    mine = pltpu.make_async_copy(
        att.at[pl.ds(pl.multiple_of(t * rows, 8), rows), :], columns(t), local_sem.at[0]
    )
    mine.start()
    between(tensor_size)
    mine.wait()
    for j in range(1, tensor_size):
        copies.receive(back[j], columns(lax.rem(t - j + tensor_size, tensor_size)), at(j))


def project_kernel(att, weight, hid, gain, out, projected, squares):
    n = pl.program_id(0)
    blocks, _, cols = projected.shape
    block = jnp.dot(att[...], weight[0], preferred_element_type=jnp.float32)
    projected[n] = block
    here = jnp.sum(block * block, axis=1, keepdims=True)

    @pl.when(n == 0)
    def _():
        squares[...] = here

    @pl.when(n > 0)
    def _():
        squares[...] += here

    @pl.when(n == blocks - 1)
    def _():
        scale = lax.rsqrt(squares[...] / (blocks * cols) + epsilon)
        for b in range(blocks):
            part = slice(b * cols, (b + 1) * cols)
            out[:, part] = (
                hid[:, part].astype(jnp.float32) + projected[b] * scale * gain[:, part]
            ).astype(out.dtype)


def local(hidden_in, q_weight, k_weight, v_weight, q_gain, k_gain, o_weight, post_gain):
    tensor_size, dp_size = lax.axis_size("tensor"), lax.axis_size("dp")
    heads_dev = q_weight.shape[1] // HD
    heads_all = heads_dev * tensor_size
    group_size = heads_all // KV_HEADS
    kv_count = max(1, heads_dev // group_size)
    k_share = min(1.0, heads_dev / group_size)
    q_width, kv_width = heads_dev * HD, kv_count * HD
    width = q_width + 2 * kv_width
    rows, model = hidden_in.shape
    depth = q_weight.shape[0]
    o_rows, o_cols = o_weight.shape
    seq_len = rows * tensor_size
    ny, nx = plane_of(tensor_size)
    nz = dp_size // CORES
    any_space = pl.BlockSpec(memory_space=pl.ANY)
    vmem = pl.BlockSpec(memory_space=pltpu.VMEM)
    bf16 = jnp.bfloat16

    per_plane = (nx - 1) + (ny - 1) + nx * (ny - 1) + ny * (nx - 1)
    slots = 4 * (nz - 1) + 2 * nz * per_plane + 2 * (2 * nz - 1) + 2 * tensor_size
    o_full, attended = pl.pallas_call(
        functools.partial(
            layer_kernel, (ny, nx, nz, heads_dev, kv_count, group_size, k_share)
        ),
        out_shape=(
            jax.ShapeDtypeStruct((dp_size, o_rows * tensor_size, o_cols), bf16),
            jax.ShapeDtypeStruct((rows, q_width * tensor_size), bf16),
        ),
        in_specs=[any_space] * 5 + [vmem] * 2,
        out_specs=(any_space,) * 2,
        scratch_shapes=[
            pltpu.VMEM((seq_len, model), bf16),
            pltpu.VMEM((depth * dp_size, width), bf16),
            pltpu.VMEM((o_rows, o_cols), bf16),
            pltpu.VMEM((seq_len, width), jnp.float32),
            pltpu.VMEM((tensor_size, 8, seq_len), jnp.float32),
            pltpu.VMEM((seq_len, q_width), bf16),
            pltpu.VMEM((seq_len, kv_width), bf16),
            pltpu.VMEM((seq_len, kv_width), bf16),
            pltpu.VMEM((seq_len, q_width), bf16),
            pltpu.SemaphoreType.DMA((5,)),
            pltpu.SemaphoreType.DMA((slots,)),
            pltpu.SemaphoreType.DMA((slots,)),
        ],
        compiler_params=pltpu.CompilerParams(collective_id=0, has_side_effects=True),
        name="layer",
    )(hidden_in, q_weight, k_weight, v_weight, o_weight, q_gain[None], k_gain[None])

    return pl.pallas_call(
        project_kernel,
        out_shape=jax.ShapeDtypeStruct((rows, model), bf16),
        grid=(dp_size,),
        in_specs=[
            pl.BlockSpec(attended.shape, lambda n: (0, 0)),
            pl.BlockSpec((1,) + o_full.shape[1:], lambda n: (n, 0, 0)),
            pl.BlockSpec((rows, model), lambda n: (0, 0)),
            pl.BlockSpec((1, model), lambda n: (0, 0)),
        ],
        out_specs=pl.BlockSpec((rows, model), lambda n: (0, 0)),
        scratch_shapes=[
            pltpu.VMEM((dp_size, rows, o_cols), jnp.float32),
            pltpu.VMEM((rows, 1), jnp.float32),
        ],
        name="project",
    )(attended, o_full, hidden_in, post_gain[None])


def solution(mesh):
    in_specs = (
        P(("dp", "tensor"), None),
        P("dp", "tensor"),
        P("dp", None),
        P("dp", None),
        P("tensor"),
        P(),
        P("tensor", "dp"),
        P(),
    )
    out_specs = P(("dp", "tensor"), None)
    return jax.shard_map(local, mesh=mesh, in_specs=in_specs, out_specs=out_specs, check_vma=False)
```

```python
import functools

import jax
import jax.numpy as jnp
from jax import lax
from jax.experimental import pallas as pl
from jax.experimental.pallas import tpu as pltpu
from jax.sharding import PartitionSpec as P

HD = 128
KV_HEADS = 8
CORES = 2
MESH = pl.DeviceIdType.MESH

epsilon = 1e-06


def plane_of(tensor_size):
    ny = max(n for n in range(1, tensor_size + 1) if tensor_size % n == 0 and n * n <= tensor_size)
    return ny, tensor_size // ny


class Copies:
    def __init__(self, send_sem, recv_sem):
        self.send_sem, self.recv_sem, self.count, self.sent = send_sem, recv_sem, 0, []

    def slot(self):
        self.count += 1
        return self.count - 1

    def make(self, slot, src, dst, device):
        return pltpu.make_async_remote_copy(
            src_ref=src,
            dst_ref=dst,
            send_sem=self.send_sem.at[slot],
            recv_sem=self.recv_sem.at[slot],
            device_id=device,
            device_id_type=MESH,
        )

    def send(self, slot, src, dst, device, when=None):
        copy = self.make(slot, src, dst, device)
        self.sent.append((copy, when))
        run(when, copy.start)

    def receive(self, slot, dst, device, when=None):
        run(when, self.make(slot, dst, dst, device).wait_recv)

    def finish(self):
        for copy, when in self.sent:
            run(when, copy.wait_send)


def run(when, action):
    if when is None:
        action()
    else:
        pl.when(when)(action)


def layer_kernel(
    plan,
    hid,
    qw,
    kw,
    vw,
    ow,
    q_gain,
    k_gain,
    full,
    out,
    tok,
    wts,
    o_v,
    qkv,
    sums,
    q_bf,
    k_bf,
    v_bf,
    att,
    local_sem,
    send_sem,
    recv_sem,
):
    ny, nx, nz, heads_dev, kv_count, group, k_share = plan
    q_width, kv_width = heads_dev * HD, kv_count * HD
    tensor_size = ny * nx
    t, d = lax.axis_index("tensor"), lax.axis_index("dp")
    tx, ty = lax.rem(t, nx), lax.div(t, nx)
    c, z = lax.rem(d, CORES), lax.div(d, CORES)
    rows, depth = hid.shape[0], qw.shape[0]
    o_rows, o_cols = ow.shape
    copies = Copies(send_sem, recv_sem)

    def at_x(j):
        return {"tensor": ty * nx + lax.rem(tx + j, nx), "dp": d}

    def at_y(j):
        return {"tensor": lax.rem(ty + j, ny) * nx + tx, "dp": d}

    up = {"tensor": t, "dp": jnp.minimum(d + CORES, nz * CORES - 1)}
    down = {"tensor": t, "dp": jnp.maximum(d - CORES, 0)}
    partner = {"tensor": t, "dp": z * CORES + 1 - c}
    has_up, has_down = z + 1 < nz, z > 0

    kv_first = pl.multiple_of(lax.div(t * heads_dev, group) * HD, HD)
    w_rows = pl.ds(pl.multiple_of(d * depth, 8), depth)
    loads = [
        pltpu.make_async_copy(qw, wts.at[w_rows, pl.ds(0, q_width)], local_sem.at[0]),
        pltpu.make_async_copy(
            kw.at[:, pl.ds(kv_first, kv_width)],
            wts.at[w_rows, pl.ds(q_width, kv_width)],
            local_sem.at[1],
        ),
        pltpu.make_async_copy(
            vw.at[:, pl.ds(kv_first, kv_width)],
            wts.at[w_rows, pl.ds(q_width + kv_width, kv_width)],
            local_sem.at[2],
        ),
        pltpu.make_async_copy(
            hid, tok.at[pl.ds(pl.multiple_of(t * rows, 8), rows), :], local_sem.at[3]
        ),
        pltpu.make_async_copy(ow, o_v, local_sem.at[4]),
    ]
    for load in loads:
        load.start()

    barrier = pltpu.get_barrier_semaphore()

    def greet(device):
        pl.semaphore_signal(barrier, inc=1, device_id=device, device_id_type=MESH)

    for j in range(1, tensor_size):
        greet({"tensor": lax.rem(t + j, tensor_size), "dp": d})
    greet(partner)
    run(has_up, lambda: greet(up))
    run(has_down, lambda: greet(down))
    pl.semaphore_wait(
        barrier, tensor_size + has_up.astype(jnp.int32) + has_down.astype(jnp.int32)
    )

    def w_at(dp):
        return wts.at[pl.ds(pl.multiple_of(dp * depth, 8), depth), :]

    def o_at(tensor, dp, part=None):
        size = o_rows if part is None else o_rows // 2
        start = tensor * o_rows + (0 if part is None else part * size)
        return full.at[dp, pl.ds(pl.multiple_of(start, 8), size), :]

    def tok_at(tensor, part):
        size = rows // 2
        return tok.at[pl.ds(pl.multiple_of(tensor * rows + part * size, 8), size), :]

    for load in loads:
        load.wait()
    line = {}
    for name in ("w", "o"):
        for way in ("up", "down"):
            for s in range(1, nz):
                line[name, way, s] = copies.slot()
    links = (("up", up, has_up, 1), ("down", down, has_down, -1))
    for way, device, has, sign in links:
        copies.send(line["w", way, 1], w_at(d), w_at(d), device, has)

    class Plane:
        def __init__(self, at, when=None):
            self.at, self.when = at, when
            self.first = {(p, j): copies.slot() for p in (0, 1) for j in range(1, (nx, ny)[p])}
            self.second = {
                (p, i, j): copies.slot()
                for p in (0, 1)
                for i in range((nx, ny)[p])
                for j in range(1, (ny, nx)[p])
            }

        def source(self, part, i):
            if part == 0:
                return ty * nx + lax.rem(tx - i + nx, nx)
            return lax.rem(ty - i + ny, ny) * nx + tx

        def start(self, src):
            for p in (0, 1):
                for j in range(1, (nx, ny)[p]):
                    copies.send(
                        self.first[p, j], src(p), self.at(t, p), (at_x, at_y)[p](j), self.when
                    )
            for p in (0, 1):
                self.cross(p, 0, src(p))

        def cross(self, p, i, src):
            for j in range(1, (ny, nx)[p]):
                copies.send(
                    self.second[p, i, j],
                    src,
                    self.at(self.source(p, i), p),
                    (at_y, at_x)[p](j),
                    self.when,
                )

        def forward(self):
            for p in (0, 1):
                for i in range(1, (nx, ny)[p]):
                    block = self.at(self.source(p, i), p)
                    copies.receive(self.first[p, i], block, (at_x, at_y)[p](i), self.when)
                    self.cross(p, i, block)

        def finish(self, diagonal=None):
            for p in (0, 1):
                for i in range((nx, ny)[p]):
                    for j in range(1, (ny, nx)[p]):
                        if diagonal is not None and diagonal != (i > 0):
                            continue
                        jx, jy = (i, j) if p == 0 else (j, i)
                        copies.receive(
                            self.second[p, i, j], self.at(near(jx, jy), p), (at_y, at_x)[p](j), self.when
                        )

    def near(jx, jy):
        return lax.rem(ty - jy + ny, ny) * nx + lax.rem(tx - jx + nx, nx)

    tokens = Plane(tok_at)
    tokens.start(lambda p: tok_at(t, p))
    to_partner = {("w", s): copies.slot() for s in range(1 - nz, nz)}
    copies.send(to_partner["w", 0], w_at(d), w_at(d), partner)
    store = pltpu.make_async_copy(o_v, o_at(t, d), local_sem.at[4])
    store.start()

    def pass_on(name, place, s):
        for way, device, has, sign in links:
            here = (z >= s) if way == "up" else (z + s < nz)
            dp = jnp.clip(d - sign * s * CORES, 0, nz * CORES - 1)
            block = place(dp)
            copies.receive(line[name, way, s], block, device, here)
            if s + 1 < nz:
                copies.send(line[name, way, s + 1], block, block, device, here & has)
            if name == "w":
                copies.send(to_partner["w", sign * s], block, block, partner, here)

    def o_place(dp):
        return o_at(t, dp)

    groups = [[] for _ in range(nz)]

    def spread(step, way=None):
        sign = -1 if way == "down" else 1
        dp = jnp.clip(d - sign * step * CORES, 0, nz * CORES - 1)
        when = None if step == 0 else (z >= step) if way == "up" else (z + step < nz)
        plane = Plane(lambda tensor, p: o_at(tensor, dp, p), when)
        half = o_rows // 2
        if step == 0:
            plane.start(lambda p: o_v.at[pl.ds(p * half, half), :])
        else:
            plane.start(lambda p: o_at(t, dp, p))
        groups[step].append((plane, sign * step))

    for s in range(1, nz):
        if s == nz - 1:
            for way, device, has, sign in links:
                copies.send(line["o", way, 1], o_v, o_at(t, d), device, has)
        pass_on("w", w_at, s)
        if s == 1:
            tokens.forward()
            spread(0)
    store.wait()
    copies.receive(to_partner["w", 0], w_at(z * CORES + 1 - c), partner)
    for s in range(1, nz):
        for way, device, has, sign in links:
            here = (z >= s) if way == "up" else (z + s < nz)
            dp = jnp.clip(z - sign * s, 0, nz - 1) * CORES + 1 - c
            copies.receive(to_partner["w", sign * s], w_at(dp), partner, here)

    width = wts.shape[1]
    step_cols = 2 * HD if width % (2 * HD) == 0 else HD

    def multiply(tensor):
        block = pl.ds(pl.multiple_of(tensor * rows, 8), rows)

        def one(n, carry):
            cols = pl.ds(pl.multiple_of(n * step_cols, HD), step_cols)
            qkv[block, cols] = jnp.dot(
                tok[block, :], wts[:, cols], preferred_element_type=jnp.float32
            )
            return carry

        lax.fori_loop(0, width // step_cols, one, 0)

    multiply(t)
    tokens.finish(diagonal=False)
    for jx in range(1, nx):
        multiply(near(jx, 0))
    for jy in range(1, ny):
        multiply(near(0, jy))
    for s in range(1, nz):
        pass_on("o", o_place, s)
    tokens.finish(diagonal=True)
    for jx in range(1, nx):
        for jy in range(1, ny):
            multiply(near(jx, jy))

    def sums_sent():
        for s in range(1, nz):
            for way, *_ in links:
                spread(s, way)

    def between(i):
        for s in range(nz):
            if i == (tensor_size if s == nz - 1 else s * tensor_size // nz):
                for plane, _ in groups[s]:
                    plane.forward()

    arrived = attend(
        (tensor_size, heads_dev, kv_count, heads_dev * tensor_size, k_share),
        copies,
        sums_sent,
        between,
        qkv,
        q_gain,
        k_gain,
        kv_first,
        out,
        sums,
        q_bf,
        k_bf,
        v_bf,
        att,
        local_sem,
    )
    column_slots = {}
    for group in groups:
        for plane, step in group:
            plane.finish()
            column_slots[step] = copies.slot()
            column = full.at[jnp.clip(d - step * CORES, 0, nz * CORES - 1)]
            copies.send(column_slots[step], column, column, partner, plane.when)
    for group in groups:
        for plane, step in group:
            column = full.at[jnp.clip(z - step, 0, nz - 1) * CORES + 1 - c]
            copies.receive(column_slots[step], column, partner, plane.when)
    arrived()
    copies.finish()


def attend(
    plan,
    copies,
    sums_sent,
    between,
    qkv,
    q_gain,
    k_gain,
    kv_first,
    out,
    sums,
    q_bf,
    k_bf,
    v_bf,
    att,
    local_sem,
):
    tensor_size, heads_dev, kv_count, heads_all, k_share = plan
    t, d = lax.axis_index("tensor"), lax.axis_index("dp")
    q_width, kv_width = heads_dev * HD, kv_count * HD
    seq_len = qkv.shape[0]
    rows = seq_len // tensor_size
    send_sem, recv_sem = copies.send_sem, copies.recv_sem

    def at(j):
        return {"tensor": lax.rem(t + j, tensor_size), "dp": d}

    queries = qkv[:, :q_width]
    key_rows = qkv[:, q_width : q_width + kv_width]

    def row_sums(block):
        ones = jnp.ones((8, block.shape[1]), jnp.float32)
        return lax.dot_general(
            ones,
            block * block,
            (((1,), (1,)), ((), ())),
            precision=lax.Precision.HIGHEST,
            preferred_element_type=jnp.float32,
        )

    upper = lax.broadcasted_iota(jnp.int32, (8, seq_len), 0) < 4
    sums[0] = jnp.where(upper, row_sums(queries), row_sums(key_rows) * k_share)
    slots = [copies.slot() for _ in range(1, tensor_size)]
    for j in range(1, tensor_size):
        copies.send(slots[j - 1], sums.at[0], sums.at[j], at(j))
    sums_sent()
    v_bf[...] = qkv[:, q_width + kv_width :].astype(jnp.bfloat16)
    for j in range(1, tensor_size):
        copies.receive(slots[j - 1], sums.at[j], at(j))
    total = sums[0]
    for j in range(1, tensor_size):
        total = total + sums[j]

    def as_column(first):
        pick = (lax.broadcasted_iota(jnp.int32, (8, HD), 0) == first).astype(jnp.float32)
        return lax.dot_general(
            total,
            pick,
            (((0,), (0,)), ((), ())),
            precision=lax.Precision.HIGHEST,
            preferred_element_type=jnp.float32,
        )

    q_scale = lax.rsqrt(as_column(0) / (heads_all * HD) + epsilon)
    k_scale = lax.rsqrt(as_column(4) / (KV_HEADS * HD) + epsilon)
    for h in range(heads_dev):
        cols = slice(h * HD, (h + 1) * HD)
        q_bf[:, cols] = (qkv[:, cols] * q_scale * q_gain[:, cols]).astype(jnp.bfloat16)
    for g in range(kv_count):
        cols = slice(g * HD, (g + 1) * HD)
        gain = k_gain[:, pl.ds(pl.multiple_of(kv_first + g * HD, HD), HD)]
        source = slice(q_width + g * HD, q_width + (g + 1) * HD)
        k_bf[:, cols] = (qkv[:, source] * k_scale * gain).astype(jnp.bfloat16)

    def columns(tensor):
        return out.at[:, pl.ds(pl.multiple_of(tensor * q_width, HD), q_width)]

    back = [copies.slot() for _ in range(tensor_size)]
    for i in range(tensor_size):
        between(i)
        block, seen = slice(i * rows, (i + 1) * rows), (i + 1) * rows
        rows_idx = lax.broadcasted_iota(jnp.int32, (rows, seen), 0) + i * rows
        cols_idx = lax.broadcasted_iota(jnp.int32, (rows, seen), 1)
        for h in range(heads_dev):
            g = h * kv_count // heads_dev
            cols, kv_cols = slice(h * HD, (h + 1) * HD), slice(g * HD, (g + 1) * HD)
            scores = lax.dot_general(
                q_bf[block, cols],
                k_bf[:seen, kv_cols],
                (((1,), (1,)), ((), ())),
                preferred_element_type=jnp.float32,
            ) * HD ** (-0.5)
            scores = jnp.where(cols_idx <= rows_idx, scores, -1e30)
            expo = jnp.exp(scores - jnp.max(scores, axis=1, keepdims=True))
            weights = (expo * (1.0 / jnp.sum(expo, axis=1, keepdims=True))).astype(jnp.bfloat16)
            att[block, cols] = jnp.dot(
                weights, v_bf[:seen, kv_cols], preferred_element_type=jnp.float32
            ).astype(jnp.bfloat16)
        own = att.at[pl.ds(i * rows, rows), :]
        j = lax.rem(i - t + tensor_size, tensor_size)
        copy = pltpu.make_async_remote_copy(
            src_ref=own,
            dst_ref=columns(t),
            send_sem=send_sem.at[back[i]],
            recv_sem=recv_sem.at[back[0] + j],
            device_id={"tensor": i, "dp": d},
            device_id_type=MESH,
        )
        copies.sent.append((copy, t != i))
        pl.when(t != i)(copy.start)
    mine = pltpu.make_async_copy(
        att.at[pl.ds(pl.multiple_of(t * rows, 8), rows), :], columns(t), local_sem.at[0]
    )
    mine.start()
    between(tensor_size)
    mine.wait()

    def arrived():
        for j in range(1, tensor_size):
            copies.receive(back[j], columns(lax.rem(t - j + tensor_size, tensor_size)), at(j))

    return arrived


def project_kernel(att, weight, hid, gain, out, projected, squares):
    n = pl.program_id(0)
    blocks, _, cols = projected.shape
    block = jnp.dot(att[...], weight[0], preferred_element_type=jnp.float32)
    projected[n] = block
    here = jnp.sum(block * block, axis=1, keepdims=True)

    @pl.when(n == 0)
    def _():
        squares[...] = here

    @pl.when(n > 0)
    def _():
        squares[...] += here

    @pl.when(n == blocks - 1)
    def _():
        scale = lax.rsqrt(squares[...] / (blocks * cols) + epsilon)
        for b in range(blocks):
            part = slice(b * cols, (b + 1) * cols)
            out[:, part] = (
                hid[:, part].astype(jnp.float32) + projected[b] * scale * gain[:, part]
            ).astype(out.dtype)


def local(hidden_in, q_weight, k_weight, v_weight, q_gain, k_gain, o_weight, post_gain):
    tensor_size, dp_size = lax.axis_size("tensor"), lax.axis_size("dp")
    heads_dev = q_weight.shape[1] // HD
    heads_all = heads_dev * tensor_size
    group_size = heads_all // KV_HEADS
    kv_count = max(1, heads_dev // group_size)
    k_share = min(1.0, heads_dev / group_size)
    q_width, kv_width = heads_dev * HD, kv_count * HD
    width = q_width + 2 * kv_width
    rows, model = hidden_in.shape
    depth = q_weight.shape[0]
    o_rows, o_cols = o_weight.shape
    seq_len = rows * tensor_size
    ny, nx = plane_of(tensor_size)
    nz = dp_size // CORES
    any_space = pl.BlockSpec(memory_space=pl.ANY)
    vmem = pl.BlockSpec(memory_space=pltpu.VMEM)
    bf16 = jnp.bfloat16

    per_plane = (nx - 1) + (ny - 1) + nx * (ny - 1) + ny * (nx - 1)
    slots = 4 * (nz - 1) + 2 * nz * per_plane + 2 * (2 * nz - 1) + 2 * tensor_size
    o_full, attended = pl.pallas_call(
        functools.partial(
            layer_kernel, (ny, nx, nz, heads_dev, kv_count, group_size, k_share)
        ),
        out_shape=(
            jax.ShapeDtypeStruct((dp_size, o_rows * tensor_size, o_cols), bf16),
            jax.ShapeDtypeStruct((rows, q_width * tensor_size), bf16),
        ),
        in_specs=[any_space] * 5 + [vmem] * 2,
        out_specs=(any_space,) * 2,
        scratch_shapes=[
            pltpu.VMEM((seq_len, model), bf16),
            pltpu.VMEM((depth * dp_size, width), bf16),
            pltpu.VMEM((o_rows, o_cols), bf16),
            pltpu.VMEM((seq_len, width), jnp.float32),
            pltpu.VMEM((tensor_size, 8, seq_len), jnp.float32),
            pltpu.VMEM((seq_len, q_width), bf16),
            pltpu.VMEM((seq_len, kv_width), bf16),
            pltpu.VMEM((seq_len, kv_width), bf16),
            pltpu.VMEM((seq_len, q_width), bf16),
            pltpu.SemaphoreType.DMA((5,)),
            pltpu.SemaphoreType.DMA((slots,)),
            pltpu.SemaphoreType.DMA((slots,)),
        ],
        compiler_params=pltpu.CompilerParams(collective_id=0, has_side_effects=True),
        name="layer",
    )(hidden_in, q_weight, k_weight, v_weight, o_weight, q_gain[None], k_gain[None])

    return pl.pallas_call(
        project_kernel,
        out_shape=jax.ShapeDtypeStruct((rows, model), bf16),
        grid=(dp_size,),
        in_specs=[
            pl.BlockSpec(attended.shape, lambda n: (0, 0)),
            pl.BlockSpec((1,) + o_full.shape[1:], lambda n: (n, 0, 0)),
            pl.BlockSpec((rows, model), lambda n: (0, 0)),
            pl.BlockSpec((1, model), lambda n: (0, 0)),
        ],
        out_specs=pl.BlockSpec((rows, model), lambda n: (0, 0)),
        scratch_shapes=[
            pltpu.VMEM((dp_size, rows, o_cols), jnp.float32),
            pltpu.VMEM((rows, 1), jnp.float32),
        ],
        name="project",
    )(attended, o_full, hidden_in, post_gain[None])


def solution(mesh):
    in_specs = (
        P(("dp", "tensor"), None),
        P("dp", "tensor"),
        P("dp", None),
        P("dp", None),
        P("tensor"),
        P(),
        P("tensor", "dp"),
        P(),
    )
    out_specs = P(("dp", "tensor"), None)
    return jax.shard_map(local, mesh=mesh, in_specs=in_specs, out_specs=out_specs, check_vma=False)
```

```python
import functools

import jax
import jax.numpy as jnp
from jax import lax
from jax.experimental import pallas as pl
from jax.experimental.pallas import tpu as pltpu
from jax.sharding import PartitionSpec as P

HD = 128
KV_HEADS = 8
CORES = 2
MESH = pl.DeviceIdType.MESH

epsilon = 1e-06


def plane_of(tensor_size):
    ny = max(n for n in range(1, tensor_size + 1) if tensor_size % n == 0 and n * n <= tensor_size)
    return ny, tensor_size // ny


class Copies:
    def __init__(self, send_sem, recv_sem):
        self.send_sem, self.recv_sem, self.count, self.sent = send_sem, recv_sem, 0, []

    def slot(self):
        self.count += 1
        return self.count - 1

    def make(self, slot, src, dst, device):
        return pltpu.make_async_remote_copy(
            src_ref=src,
            dst_ref=dst,
            send_sem=self.send_sem.at[slot],
            recv_sem=self.recv_sem.at[slot],
            device_id=device,
            device_id_type=MESH,
        )

    def send(self, slot, src, dst, device, when=None):
        copy = self.make(slot, src, dst, device)
        self.sent.append((copy, when))
        run(when, copy.start)

    def receive(self, slot, dst, device, when=None):
        run(when, self.make(slot, dst, dst, device).wait_recv)

    def finish(self):
        for copy, when in self.sent:
            run(when, copy.wait_send)


def run(when, action):
    if when is None:
        action()
    else:
        pl.when(when)(action)


def layer_kernel(
    plan,
    hid,
    qw,
    kw,
    vw,
    ow,
    q_gain,
    k_gain,
    full,
    out,
    tok,
    wts,
    o_v,
    qkv,
    sums,
    q_bf,
    k_bf,
    v_bf,
    att,
    local_sem,
    send_sem,
    recv_sem,
):
    ny, nx, nz, heads_dev, kv_count, group, k_share = plan
    q_width, kv_width = heads_dev * HD, kv_count * HD
    tensor_size = ny * nx
    t, d = lax.axis_index("tensor"), lax.axis_index("dp")
    tx, ty = lax.rem(t, nx), lax.div(t, nx)
    c, z = lax.rem(d, CORES), lax.div(d, CORES)
    rows, depth = hid.shape[0], qw.shape[0]
    o_rows, o_cols = ow.shape
    copies = Copies(send_sem, recv_sem)

    def at_x(j):
        return {"tensor": ty * nx + lax.rem(tx + j, nx), "dp": d}

    def at_y(j):
        return {"tensor": lax.rem(ty + j, ny) * nx + tx, "dp": d}

    up = {"tensor": t, "dp": jnp.minimum(d + CORES, nz * CORES - 1)}
    down = {"tensor": t, "dp": jnp.maximum(d - CORES, 0)}
    partner = {"tensor": t, "dp": z * CORES + 1 - c}
    has_up, has_down = z + 1 < nz, z > 0

    kv_first = pl.multiple_of(lax.div(t * heads_dev, group) * HD, HD)
    w_rows = pl.ds(pl.multiple_of(d * depth, 8), depth)
    loads = [
        pltpu.make_async_copy(qw, wts.at[w_rows, pl.ds(0, q_width)], local_sem.at[0]),
        pltpu.make_async_copy(
            kw.at[:, pl.ds(kv_first, kv_width)],
            wts.at[w_rows, pl.ds(q_width, kv_width)],
            local_sem.at[1],
        ),
        pltpu.make_async_copy(
            vw.at[:, pl.ds(kv_first, kv_width)],
            wts.at[w_rows, pl.ds(q_width + kv_width, kv_width)],
            local_sem.at[2],
        ),
        pltpu.make_async_copy(
            hid, tok.at[pl.ds(pl.multiple_of(t * rows, 8), rows), :], local_sem.at[3]
        ),
        pltpu.make_async_copy(ow, o_v, local_sem.at[4]),
    ]
    for load in loads:
        load.start()

    barrier = pltpu.get_barrier_semaphore()

    def greet(device):
        pl.semaphore_signal(barrier, inc=1, device_id=device, device_id_type=MESH)

    for j in range(1, tensor_size):
        greet({"tensor": lax.rem(t + j, tensor_size), "dp": d})
    greet(partner)
    run(has_up, lambda: greet(up))
    run(has_down, lambda: greet(down))
    pl.semaphore_wait(
        barrier, tensor_size + has_up.astype(jnp.int32) + has_down.astype(jnp.int32)
    )

    def w_at(dp):
        return wts.at[pl.ds(pl.multiple_of(dp * depth, 8), depth), :]

    def o_at(tensor, dp, part=None):
        size = o_rows if part is None else o_rows // 2
        start = tensor * o_rows + (0 if part is None else part * size)
        return full.at[dp, pl.ds(pl.multiple_of(start, 8), size), :]

    def tok_at(tensor, part):
        size = rows // 2
        return tok.at[pl.ds(pl.multiple_of(tensor * rows + part * size, 8), size), :]

    for load in loads:
        load.wait()
    line = {}
    for name in ("w", "o"):
        for way in ("up", "down"):
            for s in range(1, nz):
                line[name, way, s] = copies.slot()
    links = (("up", up, has_up, 1), ("down", down, has_down, -1))
    for way, device, has, sign in links:
        copies.send(line["w", way, 1], w_at(d), w_at(d), device, has)

    class Plane:
        def __init__(self, at, when=None):
            self.at, self.when = at, when
            self.first = {(p, j): copies.slot() for p in (0, 1) for j in range(1, (nx, ny)[p])}
            self.second = {
                (p, i, j): copies.slot()
                for p in (0, 1)
                for i in range((nx, ny)[p])
                for j in range(1, (ny, nx)[p])
            }

        def source(self, part, i):
            if part == 0:
                return ty * nx + lax.rem(tx - i + nx, nx)
            return lax.rem(ty - i + ny, ny) * nx + tx

        def start(self, src):
            for p in (0, 1):
                for j in range(1, (nx, ny)[p]):
                    copies.send(
                        self.first[p, j], src(p), self.at(t, p), (at_x, at_y)[p](j), self.when
                    )
            for p in (0, 1):
                self.cross(p, 0, src(p))

        def cross(self, p, i, src):
            for j in range(1, (ny, nx)[p]):
                copies.send(
                    self.second[p, i, j],
                    src,
                    self.at(self.source(p, i), p),
                    (at_y, at_x)[p](j),
                    self.when,
                )

        def forward(self):
            for p in (0, 1):
                for i in range(1, (nx, ny)[p]):
                    block = self.at(self.source(p, i), p)
                    copies.receive(self.first[p, i], block, (at_x, at_y)[p](i), self.when)
                    self.cross(p, i, block)

        def finish(self, diagonal=None):
            for p in (0, 1):
                for i in range((nx, ny)[p]):
                    for j in range(1, (ny, nx)[p]):
                        if diagonal is not None and diagonal != (i > 0):
                            continue
                        jx, jy = (i, j) if p == 0 else (j, i)
                        copies.receive(
                            self.second[p, i, j], self.at(near(jx, jy), p), (at_y, at_x)[p](j), self.when
                        )

    def near(jx, jy):
        return lax.rem(ty - jy + ny, ny) * nx + lax.rem(tx - jx + nx, nx)

    tokens = Plane(tok_at)
    tokens.start(lambda p: tok_at(t, p))
    to_partner = {("w", s): copies.slot() for s in range(1 - nz, nz)}
    copies.send(to_partner["w", 0], w_at(d), w_at(d), partner)
    store = pltpu.make_async_copy(o_v, o_at(t, d), local_sem.at[4])
    store.start()

    def pass_on(name, place, s):
        for way, device, has, sign in links:
            here = (z >= s) if way == "up" else (z + s < nz)
            dp = jnp.clip(d - sign * s * CORES, 0, nz * CORES - 1)
            block = place(dp)
            copies.receive(line[name, way, s], block, device, here)
            if s + 1 < nz:
                copies.send(line[name, way, s + 1], block, block, device, here & has)
            if name == "w":
                copies.send(to_partner["w", sign * s], block, block, partner, here)

    def o_place(dp):
        return o_at(t, dp)

    groups = [[] for _ in range(nz)]

    def spread(step, way=None):
        sign = -1 if way == "down" else 1
        dp = jnp.clip(d - sign * step * CORES, 0, nz * CORES - 1)
        when = None if step == 0 else (z >= step) if way == "up" else (z + step < nz)
        plane = Plane(lambda tensor, p: o_at(tensor, dp, p), when)
        half = o_rows // 2
        if step == 0:
            plane.start(lambda p: o_v.at[pl.ds(p * half, half), :])
        else:
            plane.start(lambda p: o_at(t, dp, p))
        groups[step].append((plane, sign * step))

    for s in range(1, nz):
        if s == nz - 1:
            for way, device, has, sign in links:
                copies.send(line["o", way, 1], o_v, o_at(t, d), device, has)
        pass_on("w", w_at, s)
        if s == 1:
            tokens.forward()
            spread(0)
    store.wait()
    copies.receive(to_partner["w", 0], w_at(z * CORES + 1 - c), partner)
    for s in range(1, nz):
        for way, device, has, sign in links:
            here = (z >= s) if way == "up" else (z + s < nz)
            dp = jnp.clip(z - sign * s, 0, nz - 1) * CORES + 1 - c
            copies.receive(to_partner["w", sign * s], w_at(dp), partner, here)

    width = wts.shape[1]
    step_cols = 2 * HD if width % (2 * HD) == 0 else HD

    def multiply(tensor):
        block = pl.ds(pl.multiple_of(tensor * rows, 8), rows)

        def one(n, carry):
            cols = pl.ds(pl.multiple_of(n * step_cols, HD), step_cols)
            qkv[block, cols] = jnp.dot(
                tok[block, :], wts[:, cols], preferred_element_type=jnp.float32
            )
            return carry

        lax.fori_loop(0, width // step_cols, one, 0)

    multiply(t)
    tokens.finish(diagonal=False)
    for jx in range(1, nx):
        multiply(near(jx, 0))
    for jy in range(1, ny):
        multiply(near(0, jy))
    for s in range(1, nz):
        pass_on("o", o_place, s)
    tokens.finish(diagonal=True)
    for jx in range(1, nx):
        for jy in range(1, ny):
            multiply(near(jx, jy))

    def sums_sent():
        for s in range(1, nz):
            for way, *_ in links:
                spread(s, way)

    def between(i):
        for s in range(nz):
            if i == (tensor_size if s == nz - 1 else s * tensor_size // nz):
                for plane, _ in groups[s]:
                    plane.forward()

    arrived = attend(
        (tensor_size, heads_dev, kv_count, heads_dev * tensor_size, k_share),
        copies,
        sums_sent,
        between,
        qkv,
        q_gain,
        k_gain,
        kv_first,
        out,
        sums,
        q_bf,
        k_bf,
        v_bf,
        att,
        local_sem,
    )
    column_slots = {}
    for group in groups:
        for plane, step in group:
            plane.finish()
            column_slots[step] = copies.slot()
            column = full.at[jnp.clip(d - step * CORES, 0, nz * CORES - 1)]
            copies.send(column_slots[step], column, column, partner, plane.when)
    for group in groups:
        for plane, step in group:
            column = full.at[jnp.clip(z - step, 0, nz - 1) * CORES + 1 - c]
            copies.receive(column_slots[step], column, partner, plane.when)
    arrived()
    copies.finish()


def attend(
    plan,
    copies,
    sums_sent,
    between,
    qkv,
    q_gain,
    k_gain,
    kv_first,
    out,
    sums,
    q_bf,
    k_bf,
    v_bf,
    att,
    local_sem,
):
    tensor_size, heads_dev, kv_count, heads_all, k_share = plan
    t, d = lax.axis_index("tensor"), lax.axis_index("dp")
    q_width, kv_width = heads_dev * HD, kv_count * HD
    seq_len = qkv.shape[0]
    rows = seq_len // tensor_size
    send_sem, recv_sem = copies.send_sem, copies.recv_sem

    def at(j):
        return {"tensor": lax.rem(t + j, tensor_size), "dp": d}

    queries = qkv[:, :q_width]
    key_rows = qkv[:, q_width : q_width + kv_width]

    def row_sums(block):
        ones = jnp.ones((8, block.shape[1]), jnp.float32)
        return lax.dot_general(
            ones,
            block * block,
            (((1,), (1,)), ((), ())),
            precision=lax.Precision.HIGHEST,
            preferred_element_type=jnp.float32,
        )

    upper = lax.broadcasted_iota(jnp.int32, (8, seq_len), 0) < 4
    sums[0] = jnp.where(upper, row_sums(queries), row_sums(key_rows) * k_share)
    slots = [copies.slot() for _ in range(1, tensor_size)]
    for j in range(1, tensor_size):
        copies.send(slots[j - 1], sums.at[0], sums.at[j], at(j))
    sums_sent()
    v_bf[...] = qkv[:, q_width + kv_width :].astype(jnp.bfloat16)
    for j in range(1, tensor_size):
        copies.receive(slots[j - 1], sums.at[j], at(j))
    total = sums[0]
    for j in range(1, tensor_size):
        total = total + sums[j]

    def as_column(first):
        pick = (lax.broadcasted_iota(jnp.int32, (8, HD), 0) == first).astype(jnp.float32)
        return lax.dot_general(
            total,
            pick,
            (((0,), (0,)), ((), ())),
            precision=lax.Precision.HIGHEST,
            preferred_element_type=jnp.float32,
        )

    q_scale = lax.rsqrt(as_column(0) / (heads_all * HD) + epsilon)
    k_scale = lax.rsqrt(as_column(4) / (KV_HEADS * HD) + epsilon)
    for h in range(heads_dev):
        cols = slice(h * HD, (h + 1) * HD)
        q_bf[:, cols] = (qkv[:, cols] * q_scale * q_gain[:, cols]).astype(jnp.bfloat16)
    for g in range(kv_count):
        cols = slice(g * HD, (g + 1) * HD)
        gain = k_gain[:, pl.ds(pl.multiple_of(kv_first + g * HD, HD), HD)]
        source = slice(q_width + g * HD, q_width + (g + 1) * HD)
        k_bf[:, cols] = (qkv[:, source] * k_scale * gain).astype(jnp.bfloat16)

    def columns(tensor):
        return out.at[:, pl.ds(pl.multiple_of(tensor * q_width, HD), q_width)]

    back = [copies.slot() for _ in range(tensor_size)]
    for i in range(tensor_size):
        between(i)
        block, seen = slice(i * rows, (i + 1) * rows), (i + 1) * rows
        rows_idx = lax.broadcasted_iota(jnp.int32, (rows, seen), 0) + i * rows
        cols_idx = lax.broadcasted_iota(jnp.int32, (rows, seen), 1)
        for h in range(heads_dev):
            g = h * kv_count // heads_dev
            cols, kv_cols = slice(h * HD, (h + 1) * HD), slice(g * HD, (g + 1) * HD)
            scores = lax.dot_general(
                q_bf[block, cols],
                k_bf[:seen, kv_cols],
                (((1,), (1,)), ((), ())),
                preferred_element_type=jnp.float32,
            ) * HD ** (-0.5)
            scores = jnp.where(cols_idx <= rows_idx, scores, -1e30)
            expo = jnp.exp(scores - jnp.max(scores, axis=1, keepdims=True))
            weights = (expo * (1.0 / jnp.sum(expo, axis=1, keepdims=True))).astype(jnp.bfloat16)
            att[block, cols] = jnp.dot(
                weights, v_bf[:seen, kv_cols], preferred_element_type=jnp.float32
            ).astype(jnp.bfloat16)
        own = att.at[pl.ds(i * rows, rows), :]
        j = lax.rem(i - t + tensor_size, tensor_size)
        copy = pltpu.make_async_remote_copy(
            src_ref=own,
            dst_ref=columns(t),
            send_sem=send_sem.at[back[i]],
            recv_sem=recv_sem.at[back[0] + j],
            device_id={"tensor": i, "dp": d},
            device_id_type=MESH,
        )
        copies.sent.append((copy, t != i))
        pl.when(t != i)(copy.start)
    mine = pltpu.make_async_copy(
        att.at[pl.ds(pl.multiple_of(t * rows, 8), rows), :], columns(t), local_sem.at[0]
    )
    mine.start()
    between(tensor_size)
    mine.wait()

    def arrived():
        for j in range(1, tensor_size):
            copies.receive(back[j], columns(lax.rem(t - j + tensor_size, tensor_size)), at(j))

    return arrived


def project_kernel(att, weight, hid, gain, out, projected, squares):
    n = pl.program_id(0)
    blocks, _, cols = projected.shape
    each = weight.shape[0]
    here = 0.0
    for b in range(each):
        block = jnp.dot(att[...], weight[b], preferred_element_type=jnp.float32)
        projected[n * each + b] = block
        here = here + jnp.sum(block * block, axis=1, keepdims=True)

    @pl.when(n == 0)
    def _():
        squares[...] = here

    @pl.when(n > 0)
    def _():
        squares[...] += here

    @pl.when(n == blocks // each - 1)
    def _():
        scale = lax.rsqrt(squares[...] / (blocks * cols) + epsilon)
        for b in range(blocks):
            part = slice(b * cols, (b + 1) * cols)
            out[:, part] = (
                hid[:, part].astype(jnp.float32) + projected[b] * scale * gain[:, part]
            ).astype(out.dtype)


def local(hidden_in, q_weight, k_weight, v_weight, q_gain, k_gain, o_weight, post_gain):
    tensor_size, dp_size = lax.axis_size("tensor"), lax.axis_size("dp")
    heads_dev = q_weight.shape[1] // HD
    heads_all = heads_dev * tensor_size
    group_size = heads_all // KV_HEADS
    kv_count = max(1, heads_dev // group_size)
    k_share = min(1.0, heads_dev / group_size)
    q_width, kv_width = heads_dev * HD, kv_count * HD
    width = q_width + 2 * kv_width
    rows, model = hidden_in.shape
    depth = q_weight.shape[0]
    o_rows, o_cols = o_weight.shape
    seq_len = rows * tensor_size
    ny, nx = plane_of(tensor_size)
    nz = dp_size // CORES
    any_space = pl.BlockSpec(memory_space=pl.ANY)
    vmem = pl.BlockSpec(memory_space=pltpu.VMEM)
    bf16 = jnp.bfloat16

    per_plane = (nx - 1) + (ny - 1) + nx * (ny - 1) + ny * (nx - 1)
    slots = 4 * (nz - 1) + 2 * nz * per_plane + 2 * (2 * nz - 1) + 2 * tensor_size
    o_full, attended = pl.pallas_call(
        functools.partial(
            layer_kernel, (ny, nx, nz, heads_dev, kv_count, group_size, k_share)
        ),
        out_shape=(
            jax.ShapeDtypeStruct((dp_size, o_rows * tensor_size, o_cols), bf16),
            jax.ShapeDtypeStruct((rows, q_width * tensor_size), bf16),
        ),
        in_specs=[any_space] * 5 + [vmem] * 2,
        out_specs=(any_space,) * 2,
        scratch_shapes=[
            pltpu.VMEM((seq_len, model), bf16),
            pltpu.VMEM((depth * dp_size, width), bf16),
            pltpu.VMEM((o_rows, o_cols), bf16),
            pltpu.VMEM((seq_len, width), jnp.float32),
            pltpu.VMEM((tensor_size, 8, seq_len), jnp.float32),
            pltpu.VMEM((seq_len, q_width), bf16),
            pltpu.VMEM((seq_len, kv_width), bf16),
            pltpu.VMEM((seq_len, kv_width), bf16),
            pltpu.VMEM((seq_len, q_width), bf16),
            pltpu.SemaphoreType.DMA((5,)),
            pltpu.SemaphoreType.DMA((slots,)),
            pltpu.SemaphoreType.DMA((slots,)),
        ],
        compiler_params=pltpu.CompilerParams(collective_id=0, has_side_effects=True),
        name="layer",
    )(hidden_in, q_weight, k_weight, v_weight, o_weight, q_gain[None], k_gain[None])

    return pl.pallas_call(
        project_kernel,
        out_shape=jax.ShapeDtypeStruct((rows, model), bf16),
        grid=(dp_size // CORES,),
        in_specs=[
            pl.BlockSpec(attended.shape, lambda n: (0, 0)),
            pl.BlockSpec((CORES,) + o_full.shape[1:], lambda n: (n, 0, 0)),
            pl.BlockSpec((rows, model), lambda n: (0, 0)),
            pl.BlockSpec((1, model), lambda n: (0, 0)),
        ],
        out_specs=pl.BlockSpec((rows, model), lambda n: (0, 0)),
        scratch_shapes=[
            pltpu.VMEM((dp_size, rows, o_cols), jnp.float32),
            pltpu.VMEM((rows, 1), jnp.float32),
        ],
        name="project",
    )(attended, o_full, hidden_in, post_gain[None])


def solution(mesh):
    in_specs = (
        P(("dp", "tensor"), None),
        P("dp", "tensor"),
        P("dp", None),
        P("dp", None),
        P("tensor"),
        P(),
        P("tensor", "dp"),
        P(),
    )
    out_specs = P(("dp", "tensor"), None)
    return jax.shard_map(local, mesh=mesh, in_specs=in_specs, out_specs=out_specs, check_vma=False)
```
